768 devices in a mesh: dp: 192 (over z_lo, x, y, core), seq: 4 (over z_hi).
Axes of the slice: x: 4, y: 8, z: 12 (z_hi: 4, z_lo: 3; z = z_hi * 3 + z_lo), core: 2. Of those that a mesh axis runs over, the one named last changes fastest.
Arguments:
- img_q_raw: bfloat16 [192, 512, 1536], P('dp', 'seq'), may hold values from -12 to 12
- img_k_raw: bfloat16 [192, 512, 1536], P('dp', 'seq'), may hold values from -6 to 6
- img_v: bfloat16 [192, 512, 1536], P('dp', 'seq'), may hold values from -6 to 6
- img_dout: bfloat16 [192, 512, 1536], P('dp', 'seq'), may hold values from -6 to 6
- txt_q_raw: bfloat16 [192, 64, 1536], P('dp', 'seq'), may hold values from -6 to 6
- txt_k_raw: bfloat16 [192, 64, 1536], P('dp'), may hold values from -6 to 6
- txt_v: bfloat16 [192, 64, 1536], P('dp'), may hold values from -6 to 6
- txt_dout: bfloat16 [192, 64, 1536], P('dp', 'seq'), may hold values from -6 to 6
- q_gain: float32 [128], replicated, may hold values from 0.6 to 3.8
- k_gain: float32 [128], replicated, may hold values from 0.6 to 3.8
Outputs:
- img_dq: bfloat16 [192, 512, 1536], P('dp', 'seq')
- img_dk: bfloat16 [192, 512, 1536], P('dp', 'seq')
- img_dv: bfloat16 [192, 512, 1536], P('dp', 'seq')
- txt_dq: bfloat16 [192, 64, 1536], P('dp', 'seq')
- txt_dk: bfloat16 [192, 64, 1536], P('dp', 'seq')
- txt_dv: bfloat16 [192, 64, 1536], P('dp', 'seq')
- q_gain_grad: float32 [128], replicated
- k_gain_grad: float32 [128], replicated
The draws below stay inside these ranges and needn't reach their ends.
All inputs are finite; a program needn't handle non-finite values.
Results may differ from the reference program's by a relative error of at most 0.012.
The reference program's roundings to bfloat16 on the way count: a program that leaves them out, or rounds other values in their place, can miss the bound.
Values may be sent and summed in bfloat16 or wider, within the bound.
A program may use at most 64 MiB of HBM per device.

```python
import jax
import jax.numpy as jnp
from jax import lax

HEADS = 12
HEAD_DIM = 128
IMG_DEV = 128
TEXT = 64
IMAGE = 512
BATCH = 192
N_SEQ = 4


def joint_image(key):
    base = jax.random.fold_in(key, 7)
    first_key, second_key = jax.random.split(base, 2)
    keys_image = jnp.clip(jax.random.normal(first_key, (BATCH, IMAGE, HEADS * HEAD_DIM), jnp.float32), -6.0, 6.0)
    queries = jnp.clip(jax.random.normal(second_key, (BATCH, IMAGE, HEADS * HEAD_DIM), jnp.float32), -6.0, 6.0)
    return (queries, keys_image)


def draw_img_q_raw(key, part):
    return joint_image(key)[0].astype(jnp.bfloat16)


def draw_img_k_raw(key, part):
    return joint_image(key)[1].astype(jnp.bfloat16)


def draw_q_gain(key, part):
    base = jax.random.fold_in(key, 11)
    return jax.random.uniform(base, (HEAD_DIM,), jnp.float32, 0.6, 1.4)


def draw_k_gain(key, part):
    base = jax.random.fold_in(key, 13)
    return jax.random.uniform(base, (HEAD_DIM,), jnp.float32, 0.6, 1.4)


def steps_of(key, shape, pieces, least, high):
    def one(dim, parts):
        heights = jax.random.uniform(jax.random.fold_in(jax.random.fold_in(key, 6), dim), (parts,), jnp.float32, least / len(pieces), high / len(pieces))
        return jnp.repeat(jnp.exp(heights), shape[dim] // parts).reshape((-1,) + (1,) * (len(shape) - dim - 1))

    factor_of = one(*pieces[0])
    for cut in pieces[1:]:
        factor_of = factor_of * one(*cut)
    return factor_of


def gaussian(key, extent, deviation, most, cuts=(), dtype=jnp.bfloat16):
    factor_of = steps_of(key, extent, cuts, -0.22, 0.18) if cuts else 1.0
    array = jax.random.normal(key, extent, jnp.float32) * deviation * factor_of
    return jnp.minimum(jnp.maximum(array, -most), most).astype(dtype)


def setup_inputs(seed: int = 0) -> dict:
    splits = jax.random.split(jax.random.key(seed), 11)
    return {
        "img_q_raw": draw_img_q_raw(jax.random.fold_in(splits[10], 71), 0),
        "img_k_raw": draw_img_k_raw(jax.random.fold_in(splits[10], 71), 0),
        "img_v": gaussian(splits[2], (BATCH, IMAGE, HEADS * HEAD_DIM), 1.0, 6.0, ((0, 192), (1, 4))),
        "img_dout": gaussian(splits[3], (BATCH, IMAGE, HEADS * HEAD_DIM), 1.0, 6.0, ((0, 192), (1, 4))),
        "txt_q_raw": gaussian(splits[4], (BATCH, TEXT, HEADS * HEAD_DIM), 1.0, 6.0, ((0, 192), (1, 4))),
        "txt_k_raw": gaussian(splits[5], (BATCH, TEXT, HEADS * HEAD_DIM), 1.0, 6.0, ((0, 192),)),
        "txt_v": gaussian(splits[6], (BATCH, TEXT, HEADS * HEAD_DIM), 1.0, 6.0, ((0, 192),)),
        "txt_dout": gaussian(splits[7], (BATCH, TEXT, HEADS * HEAD_DIM), 1.0, 6.0, ((0, 192), (1, 4))),
        "q_gain": draw_q_gain(jax.random.fold_in(splits[10], 71), 0),
        "k_gain": draw_k_gain(jax.random.fold_in(splits[10], 71), 0),
    }


epsilon = 1e-06

def normalize(source, norm_gain):
    values = source.astype(jnp.float32)
    inverse = lax.rsqrt(lax.optimization_barrier(jnp.mean(values * values, axis=-1, keepdims=True)) + epsilon)
    return values * inverse * norm_gain

def rounded(values):
    return lax.optimization_barrier(values.astype(jnp.bfloat16)).astype(jnp.float32)

def blocked(image_rows, text_rows):
    image_part = image_rows.reshape(N_SEQ, IMG_DEV, HEADS, HEAD_DIM)
    text_part = text_rows.reshape(N_SEQ, TEXT // N_SEQ, HEADS, HEAD_DIM)
    return jnp.concatenate([image_part, text_part], axis=1)

def sample(q_gain, k_gain, inputs):
    img_q, img_k, img_val, img_grad, txt_q, txt_k, txt_val, txt_grad = inputs
    query_src = blocked(img_q, txt_q).astype(jnp.float32)
    dout_f = blocked(img_grad, txt_grad).astype(jnp.float32)
    key_src = jnp.concatenate([img_k, txt_k], axis=0).reshape(IMAGE + TEXT, HEADS, HEAD_DIM).astype(jnp.float32)
    value_all = jnp.concatenate([img_val, txt_val], axis=0).reshape(IMAGE + TEXT, HEADS, HEAD_DIM).astype(jnp.float32)
    query_b = rounded(normalize(query_src, q_gain))
    key_b = rounded(normalize(key_src, k_gain))
    score_scale = HEAD_DIM ** (-0.5)
    scores = jnp.einsum('nqhd,khd->nhqk', query_b, key_b) * score_scale
    row_max = lax.optimization_barrier(jnp.max(scores, axis=-1, keepdims=True))
    shifted = scores - row_max
    log_total = jnp.log(lax.optimization_barrier(jnp.sum(jnp.exp(shifted), axis=-1, keepdims=True)))
    prob_full = jnp.exp(shifted - log_total)
    probs_b = rounded(prob_full)
    output_b = rounded(jnp.einsum('nhqk,khd->nqhd', probs_b, value_all))
    dprob = jnp.einsum('nqhd,khd->nhqk', dout_f, value_all)
    row_delta = jnp.transpose(lax.optimization_barrier(jnp.sum(dout_f * output_b, axis=-1)), (0, 2, 1))[..., None]
    dscore_b = rounded(prob_full * (dprob - row_delta) * score_scale)
    dquery = jnp.einsum('nhqk,khd->nqhd', dscore_b, key_b)
    dkey = lax.optimization_barrier(jnp.sum(rounded(jnp.einsum('nhqk,nqhd->nkhd', dscore_b, query_b)), axis=0))
    dvalue = lax.optimization_barrier(jnp.sum(rounded(jnp.einsum('nhqk,nqhd->nkhd', probs_b, dout_f)), axis=0))
    result_q, query_pull = jax.vjp(normalize, query_src, q_gain)
    dquery_src, dq_gain = query_pull(dquery)
    result_k, key_pull = jax.vjp(normalize, key_src, k_gain)
    dkey_src, dk_gain = key_pull(dkey)
    width_all = HEADS * HEAD_DIM
    dq_b = dquery_src.astype(jnp.bfloat16)
    image_dq = dq_b[:, :IMG_DEV].reshape(IMAGE, width_all)
    text_dq = dq_b[:, IMG_DEV:].reshape(TEXT, width_all)
    dk_b = dkey_src.reshape(IMAGE + TEXT, width_all).astype(jnp.bfloat16)
    dv_b = dvalue.reshape(IMAGE + TEXT, width_all).astype(jnp.bfloat16)
    return (image_dq, dk_b[:IMAGE], dv_b[:IMAGE], text_dq, dk_b[IMAGE:], dv_b[IMAGE:], dq_gain, dk_gain)

def reference(img_q_raw, img_k_raw, img_v, img_dout, txt_q_raw, txt_k_raw, txt_v, txt_dout, q_gain, k_gain):

    def per_sample(inputs):
        return sample(q_gain, k_gain, inputs)
    results = lax.map(per_sample, (img_q_raw, img_k_raw, img_v, img_dout, txt_q_raw, txt_k_raw, txt_v, txt_dout))
    return (results[0], results[1], results[2], results[3], results[4], results[5], lax.optimization_barrier(jnp.sum(results[6], axis=0)), lax.optimization_barrier(jnp.sum(results[7], axis=0)))
```

```python
import functools

import jax
import jax.numpy as jnp
from jax import lax
from jax.experimental import pallas as pl
from jax.experimental.pallas import tpu as pltpu
from jax.sharding import PartitionSpec as P

HEAD_DIM = 128
EPSILON = 1e-06
DP_PARTS = (3, 4, 8, 2)
BF16 = jnp.bfloat16
F32 = jnp.float32


def axis_peers(part):
    stride = 1
    for size in DP_PARTS[part + 1 :]:
        stride *= size
    size = DP_PARTS[part]
    index = lax.axis_index("dp")
    place = lax.rem(index // stride, size)
    base = index - place * stride
    return [base + lax.rem(place + step, size) * stride for step in range(1, size)]


def dot_nt(a, b):
    return lax.dot_general(a, b, (((1,), (1,)), ((), ())), preferred_element_type=F32)


def dot_nn(a, b):
    return lax.dot_general(a, b, (((1,), (0,)), ((), ())), preferred_element_type=F32)


def dot_tn(a, b):
    return lax.dot_general(a, b, (((0,), (0,)), ((), ())), preferred_element_type=F32)


def inverse_rms(x):
    return lax.rsqrt(jnp.mean(x * x, axis=-1, keepdims=True) + EPSILON)


def norm_pull(x, gain, upstream):
    inverse = inverse_rms(x)
    unit = x * inverse
    scaled = upstream * gain
    along = jnp.mean(scaled * unit, axis=-1, keepdims=True)
    return inverse * (scaled - unit * along), upstream * unit


def exchange_kernel(
    seq_count,
    heads,
    img,
    txt,
    iq_ref,
    ik_ref,
    iv_ref,
    id_ref,
    tq_ref,
    tk_ref,
    tv_ref,
    td_ref,
    qg_ref,
    kg_ref,
    land_ref,
    gain_ref,
    stage,
    arrived,
    text_k,
    text_v,
    outgoing,
    keys,
    values,
    key_acc,
    value_acc,
    gain_src,
    gain_in,
    stage_sem,
    own_sem,
    in_send,
    in_recv,
    out_send,
    out_recv,
    own_out_sem,
    gain_send,
    gain_recv,
    gains,
):
    me = lax.axis_index("seq")
    rows = img + txt
    span = heads * HEAD_DIM
    scale = HEAD_DIM ** (-0.5)
    offsets = range(1, seq_count)
    seq_peers = [lax.rem(me + step, seq_count) for step in offsets]
    stages = [
        [{"seq": peer} for peer in seq_peers],
        [{"dp": peer} for peer in axis_peers(0)],
        [{"dp": peer} for peer in axis_peers(3)],
        [{"dp": peer} for peer in axis_peers(1)],
        [{"dp": peer} for peer in axis_peers(2)],
    ]
    barrier = pltpu.get_barrier_semaphore()
    total = 0
    for peers in stages:
        for peer in peers:
            pl.semaphore_signal(barrier, inc=1, device_id=peer, device_id_type=pl.DeviceIdType.MESH)
            total += 1

    def fetch(owner, target, sem):
        lanes = pl.ds(pl.multiple_of(owner * span, HEAD_DIM), span)
        row = 0
        for source, count in (
            (iq_ref, img),
            (tq_ref, txt),
            (id_ref, img),
            (td_ref, txt),
            (ik_ref, img),
            (iv_ref, img),
        ):
            pltpu.make_async_copy(
                source.at[0, :, lanes], target.at[pl.ds(row, count), :], sem
            ).start()
            row += count

    for step, peer in zip(offsets, seq_peers):
        fetch(peer, stage.at[step], stage_sem.at[step])
    fetch(me, stage.at[0], stage_sem.at[0])
    my_lanes = pl.ds(pl.multiple_of(me * span, HEAD_DIM), span)
    text_copies = (
        pltpu.make_async_copy(tk_ref.at[0, :, my_lanes], text_k, own_sem.at[0]),
        pltpu.make_async_copy(tv_ref.at[0, :, my_lanes], text_v, own_sem.at[1]),
        pltpu.make_async_copy(qg_ref, gains.at[pl.ds(0, 1)], own_sem.at[2]),
        pltpu.make_async_copy(kg_ref, gains.at[pl.ds(1, 1)], own_sem.at[3]),
    )
    for copy in text_copies:
        copy.start()

    def staged(step):
        return pltpu.make_async_copy(stage.at[step], stage.at[step], stage_sem.at[step])

    for step in offsets:
        staged(step).wait()
    pl.semaphore_wait(barrier, total)

    def in_copy(head, step):
        lanes = pl.ds(pl.multiple_of(head * HEAD_DIM, HEAD_DIM), HEAD_DIM)
        return pltpu.make_async_remote_copy(
            src_ref=stage.at[step, :, lanes],
            dst_ref=arrived.at[me, head],
            send_sem=in_send.at[head, step - 1],
            recv_sem=in_recv.at[head, step - 1],
            device_id={"seq": lax.rem(me + step, seq_count)},
            device_id_type=pl.DeviceIdType.MESH,
        )

    def out_copy(head, step):
        lanes = pl.ds(pl.multiple_of(head * HEAD_DIM, HEAD_DIM), HEAD_DIM)
        peer = lax.rem(me + step, seq_count)
        return pltpu.make_async_remote_copy(
            src_ref=outgoing.at[peer, head],
            dst_ref=land_ref.at[me, :, :, lanes],
            send_sem=out_send.at[head, step - 1],
            recv_sem=out_recv.at[head, step - 1],
            device_id={"seq": peer},
            device_id_type=pl.DeviceIdType.MESH,
        )

    def own_in(head):
        lanes = pl.ds(pl.multiple_of(head * HEAD_DIM, HEAD_DIM), HEAD_DIM)
        return pltpu.make_async_copy(
            stage.at[0, :, lanes], arrived.at[me, head], own_sem.at[4 + head]
        )

    def own_out(head):
        lanes = pl.ds(pl.multiple_of(head * HEAD_DIM, HEAD_DIM), HEAD_DIM)
        return pltpu.make_async_copy(
            outgoing.at[me, head], land_ref.at[me, :, :, lanes], own_out_sem.at[head]
        )

    def send_in(head, carry):
        for step in (2, 1, 3):
            in_copy(head, step).start()
        return carry

    lax.fori_loop(0, heads, send_in, 0)
    staged(0).wait()
    for copy in text_copies:
        copy.wait()

    def move_own(head, carry):
        own_in(head).start()
        return carry

    lax.fori_loop(0, heads, move_own, 0)
    q_gain = gains[0:1]
    k_gain = gains[1:2]
    do_row, k_row, v_row = rows, 2 * rows, 2 * rows + img

    def one_head(head, carry):
        q_total, k_total = carry
        own_in(head).wait()
        for step in offsets:
            in_copy(head, step).wait_recv()
        lanes = pl.ds(pl.multiple_of(head * HEAD_DIM, HEAD_DIM), HEAD_DIM)

        def raw_keys(j):
            return jnp.concatenate(
                [
                    arrived[j, head, k_row : k_row + img, :].astype(F32),
                    text_k[j * txt : (j + 1) * txt, lanes].astype(F32),
                ],
                axis=0,
            )

        for j in range(seq_count):
            x = raw_keys(j)
            keys[j] = (x * inverse_rms(x) * k_gain).astype(BF16)
            values[j, :img] = arrived[j, head, v_row : v_row + img, :]
            values[j, img:] = text_v[j * txt : (j + 1) * txt, lanes]
        kn = keys[...].reshape(seq_count * rows, HEAD_DIM)
        vv = values[...].reshape(seq_count * rows, HEAD_DIM)
        for j in range(seq_count):
            xq = arrived[j, head, :rows, :].astype(F32)
            qn = (xq * inverse_rms(xq) * q_gain).astype(BF16)
            dout = arrived[j, head, do_row : do_row + rows, :]
            scores = dot_nt(qn, kn) * scale
            weights = jnp.exp(scores - jnp.max(scores, axis=-1, keepdims=True))
            prob = weights * (1.0 / jnp.sum(weights, axis=-1, keepdims=True))
            prob_b = prob.astype(BF16)
            out_b = dot_nn(prob_b, vv).astype(BF16)
            delta = jnp.sum(dout.astype(F32) * out_b.astype(F32), axis=-1, keepdims=True)
            dscore = (prob * (dot_nt(dout, vv) - delta) * scale).astype(BF16)
            dq = dot_nn(dscore, kn)
            key_part = dot_tn(dscore, qn).astype(BF16).astype(F32)
            value_part = dot_tn(prob_b, dout).astype(BF16).astype(F32)
            if j == 0:
                key_acc[...] = key_part
                value_acc[...] = value_part
            else:
                key_acc[...] += key_part
                value_acc[...] += value_part
            dx, terms = norm_pull(xq, q_gain, dq)
            outgoing[j, head, 0] = dx.astype(BF16)
            q_total += jnp.sum(terms, axis=0, keepdims=True)
        for j in range(seq_count):
            dx, terms = norm_pull(raw_keys(j), k_gain, key_acc[j * rows : (j + 1) * rows])
            outgoing[j, head, 1] = dx.astype(BF16)
            outgoing[j, head, 2] = value_acc[j * rows : (j + 1) * rows].astype(BF16)
            k_total += jnp.sum(terms, axis=0, keepdims=True)

        @pl.when(head < heads - 1)
        def _():
            for step in (2, 1, 3):
                out_copy(head, step).start()
            own_out(head).start()

        return q_total, k_total

    zero = jnp.zeros((1, HEAD_DIM), F32)
    q_total, k_total = lax.fori_loop(0, heads, one_head, (zero, zero))
    gain = jnp.concatenate([q_total, k_total, jnp.zeros((6, HEAD_DIM), F32)], axis=0)
    slot = 0
    copies = []
    for number, peers in enumerate(stages):
        gain_src[number] = gain
        current = []
        for index, peer in enumerate(peers):
            copy = pltpu.make_async_remote_copy(
                src_ref=gain_src.at[number],
                dst_ref=gain_in.at[slot + index],
                send_sem=gain_send.at[slot + index],
                recv_sem=gain_recv.at[slot + index],
                device_id=peer,
                device_id_type=pl.DeviceIdType.MESH,
            )
            copy.start()
            current.append(copy)
        if number == 0:
            for step in (2, 1, 3):
                out_copy(heads - 1, step).start()
            own_out(heads - 1).start()
        for index, copy in enumerate(current):
            copy.wait_recv()
            gain = gain + gain_in[slot + index]
        copies += current
        slot += len(peers)
    gain_ref[...] = gain
    for copy in copies:
        copy.wait_send()

    def drain(head, carry):
        own_out(head).wait()
        for step in offsets:
            in_copy(head, step).wait_send()
            out_copy(head, step).wait()
        return carry

    lax.fori_loop(0, heads, drain, 0)


def place_kernel(seq_count, span, img, txt, land_ref, gain_ref, *refs):
    outs, sems = refs[:-1], refs[-1]
    copies = [(gain_ref.at[pl.ds(n, 1)], outs[6 + n]) for n in range(2)]
    for j in range(seq_count):
        lanes = pl.ds(j * span, span)
        for kind in range(3):
            copies.append((land_ref.at[j, kind, pl.ds(0, img)], outs[kind].at[0, :, lanes]))
            copies.append((land_ref.at[j, kind, pl.ds(img, txt)], outs[3 + kind].at[0, :, lanes]))
    started = [
        pltpu.make_async_copy(source, target, sems.at[number])
        for number, (source, target) in enumerate(copies)
    ]
    for copy in started:
        copy.start()
    for copy in started:
        copy.wait()


def local(seq_count, iq, ik, iv, idt, tq, tk, tv, td, q_gain, k_gain):
    img, lanes = iq.shape[1], iq.shape[2]
    txt = tq.shape[1]
    rows = img + txt
    heads = lanes // HEAD_DIM // seq_count
    span = heads * HEAD_DIM
    sent = 2 * rows + 2 * img
    peers = seq_count - 1 + sum(size - 1 for size in DP_PARTS)
    tokens = [
        pltpu.with_memory_space_constraint(x, pltpu.HBM)
        for x in (iq, ik, iv, idt, tq, tk, tv, td, q_gain[None], k_gain[None])
    ]
    hbm = pl.BlockSpec(memory_space=pltpu.HBM)
    vmem = pl.BlockSpec(memory_space=pltpu.VMEM)
    dma = pltpu.SemaphoreType.DMA
    land, gain = pl.pallas_call(
        functools.partial(exchange_kernel, seq_count, heads, img, txt),
        out_shape=(
            pltpu.VMEM((seq_count, 3, rows, span), BF16),
            pltpu.VMEM((8, HEAD_DIM), F32),
        ),
        in_specs=[hbm] * 10,
        out_specs=(vmem, vmem),
        scratch_shapes=[
            pltpu.VMEM((seq_count, sent, span), BF16),
            pltpu.VMEM((seq_count, heads, sent, HEAD_DIM), BF16),
            pltpu.VMEM((seq_count * txt, span), BF16),
            pltpu.VMEM((seq_count * txt, span), BF16),
            pltpu.VMEM((seq_count, heads, 3, rows, HEAD_DIM), BF16),
            pltpu.VMEM((seq_count, rows, HEAD_DIM), BF16),
            pltpu.VMEM((seq_count, rows, HEAD_DIM), BF16),
            pltpu.VMEM((seq_count * rows, HEAD_DIM), F32),
            pltpu.VMEM((seq_count * rows, HEAD_DIM), F32),
            pltpu.VMEM((1 + len(DP_PARTS), 8, HEAD_DIM), F32),
            pltpu.VMEM((peers, 8, HEAD_DIM), F32),
            dma((seq_count,)),
            dma((4 + heads,)),
            dma((heads, seq_count - 1)),
            dma((heads, seq_count - 1)),
            dma((heads, seq_count - 1)),
            dma((heads, seq_count - 1)),
            dma((heads,)),
            dma((peers,)),
            dma((peers,)),
            pltpu.VMEM((2, HEAD_DIM), F32),
        ],
        compiler_params=pltpu.CompilerParams(collective_id=0, has_side_effects=True, vmem_limit_bytes=40 << 20),
        name="exchange",
    )(*tokens)
    big = jax.ShapeDtypeStruct((1, img, lanes), BF16)
    small = jax.ShapeDtypeStruct((1, txt, lanes), BF16)
    row = jax.ShapeDtypeStruct((1, HEAD_DIM), F32)
    placed = pl.pallas_call(
        functools.partial(place_kernel, seq_count, span, img, txt),
        out_shape=(big,) * 3 + (small,) * 3 + (row,) * 2,
        in_specs=[vmem] * 2,
        out_specs=(hbm,) * 8,
        scratch_shapes=[dma((seq_count * 6 + 2,))],
        compiler_params=pltpu.CompilerParams(vmem_limit_bytes=4 << 20),
        name="place",
    )(*(pltpu.with_memory_space_constraint(x, pltpu.VMEM) for x in (land, gain)))
    return (*placed[:6], placed[6][0], placed[7][0])


def solution(mesh):
    split = P("dp", "seq", None)
    whole = P("dp", None, None)
    return jax.shard_map(
        functools.partial(local, mesh.shape["seq"]),
        mesh=mesh,
        in_specs=(split,) * 5 + (whole,) * 2 + (split, P(), P()),
        out_specs=(split,) * 6 + (P(), P()),
        check_vma=False,
    )
```

```python
import functools

import jax
import jax.numpy as jnp
from jax import lax
from jax.experimental import pallas as pl
from jax.experimental.pallas import tpu as pltpu
from jax.sharding import PartitionSpec as P

HEAD_DIM = 128
EPSILON = 1e-06
DP_PARTS = (3, 4, 8, 2)
BF16 = jnp.bfloat16
F32 = jnp.float32


def axis_peers(part):
    stride = 1
    for size in DP_PARTS[part + 1 :]:
        stride *= size
    size = DP_PARTS[part]
    index = lax.axis_index("dp")
    place = lax.rem(index // stride, size)
    base = index - place * stride
    return [{"dp": base + lax.rem(place + step, size) * stride} for step in range(1, size)]


def column_peers(seq_count):
    me = lax.axis_index("seq")
    own = [{"dp": lax.axis_index("dp")}] + axis_peers(0)
    return [
        {**lower, "seq": lax.rem(me + step, seq_count)}
        for step in range(seq_count)
        for number, lower in enumerate(own)
        if step or number
    ]


def dot_nt(a, b):
    return lax.dot_general(a, b, (((1,), (1,)), ((), ())), preferred_element_type=F32)


def dot_nn(a, b):
    return lax.dot_general(a, b, (((1,), (0,)), ((), ())), preferred_element_type=F32)


def dot_tn(a, b):
    return lax.dot_general(a, b, (((0,), (0,)), ((), ())), preferred_element_type=F32)


def inverse_rms(x):
    return lax.rsqrt(jnp.mean(x * x, axis=-1, keepdims=True) + EPSILON)


def norm_pull(x, gain, upstream):
    inverse = inverse_rms(x)
    unit = x * inverse
    scaled = upstream * gain
    along = jnp.mean(scaled * unit, axis=-1, keepdims=True)
    return inverse * (scaled - unit * along), upstream * unit


def exchange_kernel(
    seq_count,
    heads,
    img,
    txt,
    iq_ref,
    ik_ref,
    iv_ref,
    id_ref,
    tq_ref,
    tk_ref,
    tv_ref,
    td_ref,
    qg_ref,
    kg_ref,
    land_ref,
    gain_ref,
    stage,
    arrived,
    text_k,
    text_v,
    outgoing,
    keys,
    values,
    key_acc,
    value_acc,
    gain_src,
    gain_in,
    stage_sem,
    own_sem,
    in_send,
    in_recv,
    out_send,
    out_recv,
    own_out_sem,
    gain_send,
    gain_recv,
    gains,
):
    me = lax.axis_index("seq")
    rows = img + txt
    span = heads * HEAD_DIM
    scale = HEAD_DIM ** (-0.5)
    offsets = range(1, seq_count)
    seq_peers = [lax.rem(me + step, seq_count) for step in offsets]
    stages = [axis_peers(3), axis_peers(1), axis_peers(2), column_peers(seq_count)]
    barrier = pltpu.get_barrier_semaphore()
    total = 0
    for peers in reversed(stages):
        for peer in peers:
            pl.semaphore_signal(barrier, inc=1, device_id=peer, device_id_type=pl.DeviceIdType.MESH)
            total += 1

    def fetch(owner, target, sem):
        lanes = pl.ds(pl.multiple_of(owner * span, HEAD_DIM), span)
        row = 0
        for source, count in (
            (iq_ref, img),
            (tq_ref, txt),
            (id_ref, img),
            (td_ref, txt),
            (ik_ref, img),
            (iv_ref, img),
        ):
            pltpu.make_async_copy(
                source.at[0, :, lanes], target.at[pl.ds(row, count), :], sem
            ).start()
            row += count

    for step, peer in zip(offsets, seq_peers):
        fetch(peer, stage.at[step], stage_sem.at[step])
    fetch(me, stage.at[0], stage_sem.at[0])
    my_lanes = pl.ds(pl.multiple_of(me * span, HEAD_DIM), span)
    text_copies = (
        pltpu.make_async_copy(tk_ref.at[0, :, my_lanes], text_k, own_sem.at[0]),
        pltpu.make_async_copy(tv_ref.at[0, :, my_lanes], text_v, own_sem.at[1]),
        pltpu.make_async_copy(qg_ref, gains.at[pl.ds(0, 1)], own_sem.at[2]),
        pltpu.make_async_copy(kg_ref, gains.at[pl.ds(1, 1)], own_sem.at[3]),
    )
    for copy in text_copies:
        copy.start()

    def staged(step):
        return pltpu.make_async_copy(stage.at[step], stage.at[step], stage_sem.at[step])

    for step in offsets:
        staged(step).wait()
    pl.semaphore_wait(barrier, total)

    def in_copy(head, step):
        lanes = pl.ds(pl.multiple_of(head * HEAD_DIM, HEAD_DIM), HEAD_DIM)
        return pltpu.make_async_remote_copy(
            src_ref=stage.at[step, :, lanes],
            dst_ref=arrived.at[me, head],
            send_sem=in_send.at[head, step - 1],
            recv_sem=in_recv.at[head, step - 1],
            device_id={"seq": lax.rem(me + step, seq_count)},
            device_id_type=pl.DeviceIdType.MESH,
        )

    def out_copy(head, step):
        lanes = pl.ds(pl.multiple_of(head * HEAD_DIM, HEAD_DIM), HEAD_DIM)
        peer = lax.rem(me + step, seq_count)
        return pltpu.make_async_remote_copy(
            src_ref=outgoing.at[peer, head],
            dst_ref=land_ref.at[me, :, :, lanes],
            send_sem=out_send.at[head, step - 1],
            recv_sem=out_recv.at[head, step - 1],
            device_id={"seq": peer},
            device_id_type=pl.DeviceIdType.MESH,
        )

    def own_in(head):
        lanes = pl.ds(pl.multiple_of(head * HEAD_DIM, HEAD_DIM), HEAD_DIM)
        return pltpu.make_async_copy(
            stage.at[0, :, lanes], arrived.at[me, head], own_sem.at[4 + head]
        )

    def own_out(head):
        lanes = pl.ds(pl.multiple_of(head * HEAD_DIM, HEAD_DIM), HEAD_DIM)
        return pltpu.make_async_copy(
            outgoing.at[me, head], land_ref.at[me, :, :, lanes], own_out_sem.at[head]
        )

    def send_out(head):
        for number in range(seq_count - 1):
            peer = number + jnp.where(number >= me, 1, 0)
            out_copy(head, lax.rem(peer - me + seq_count, seq_count)).start()
        own_out(head).start()

    def send_in(head, carry):
        for step in (2, 1, 3):
            in_copy(head, step).start()
        return carry

    lax.fori_loop(0, heads, send_in, 0)
    staged(0).wait()
    for copy in text_copies:
        copy.wait()

    def move_own(head, carry):
        own_in(head).start()
        return carry

    lax.fori_loop(0, heads, move_own, 0)
    q_gain = gains[0:1]
    k_gain = gains[1:2]
    do_row, k_row, v_row = rows, 2 * rows, 2 * rows + img

    def one_head(head, carry):
        q_total, k_total = carry
        own_in(head).wait()
        for step in offsets:
            in_copy(head, step).wait_recv()
        lanes = pl.ds(pl.multiple_of(head * HEAD_DIM, HEAD_DIM), HEAD_DIM)

        def raw_keys(j):
            return jnp.concatenate(
                [
                    arrived[j, head, k_row : k_row + img, :].astype(F32),
                    text_k[j * txt : (j + 1) * txt, lanes].astype(F32),
                ],
                axis=0,
            )

        for j in range(seq_count):
            x = raw_keys(j)
            keys[j] = (x * inverse_rms(x) * k_gain).astype(BF16)
            values[j, :img] = arrived[j, head, v_row : v_row + img, :]
            values[j, img:] = text_v[j * txt : (j + 1) * txt, lanes]
        kn = keys[...].reshape(seq_count * rows, HEAD_DIM)
        vv = values[...].reshape(seq_count * rows, HEAD_DIM)
        for j in range(seq_count):
            xq = arrived[j, head, :rows, :].astype(F32)
            qn = (xq * inverse_rms(xq) * q_gain).astype(BF16)
            dout = arrived[j, head, do_row : do_row + rows, :]
            scores = dot_nt(qn, kn) * scale
            weights = jnp.exp(scores - jnp.max(scores, axis=-1, keepdims=True))
            prob = weights * (1.0 / jnp.sum(weights, axis=-1, keepdims=True))
            prob_b = prob.astype(BF16)
            out_b = dot_nn(prob_b, vv).astype(BF16)
            delta = jnp.sum(dout.astype(F32) * out_b.astype(F32), axis=-1, keepdims=True)
            dscore = (prob * (dot_nt(dout, vv) - delta) * scale).astype(BF16)
            dq = dot_nn(dscore, kn)
            key_part = dot_tn(dscore, qn).astype(BF16).astype(F32)
            value_part = dot_tn(prob_b, dout).astype(BF16).astype(F32)
            if j == 0:
                key_acc[...] = key_part
                value_acc[...] = value_part
            else:
                key_acc[...] += key_part
                value_acc[...] += value_part
            dx, terms = norm_pull(xq, q_gain, dq)
            outgoing[j, head, 0] = dx.astype(BF16)
            q_total += jnp.sum(terms, axis=0, keepdims=True)
        for j in range(seq_count):
            dx, terms = norm_pull(raw_keys(j), k_gain, key_acc[j * rows : (j + 1) * rows])
            outgoing[j, head, 1] = dx.astype(BF16)
            outgoing[j, head, 2] = value_acc[j * rows : (j + 1) * rows].astype(BF16)
            k_total += jnp.sum(terms, axis=0, keepdims=True)

        @pl.when(head < heads - 1)
        def _():
            send_out(head)

        return q_total, k_total

    zero = jnp.zeros((1, HEAD_DIM), F32)
    q_total, k_total = lax.fori_loop(0, heads, one_head, (zero, zero))
    gain = jnp.concatenate([q_total, k_total], axis=0)
    slot = 0
    copies = []
    for number, peers in enumerate(stages):
        gain_src[number] = gain
        current = []
        for index, peer in enumerate(peers):
            copy = pltpu.make_async_remote_copy(
                src_ref=gain_src.at[number],
                dst_ref=gain_in.at[slot + index],
                send_sem=gain_send.at[slot + index],
                recv_sem=gain_recv.at[slot + index],
                device_id=peer,
                device_id_type=pl.DeviceIdType.MESH,
            )
            copy.start()
            current.append(copy)
        if number == len(stages) - 1:
            send_out(heads - 1)
        for index, copy in enumerate(current):
            copy.wait_recv()
            gain = gain + gain_in[slot + index]
        copies += current
        slot += len(peers)
    gain_ref[...] = gain
    for copy in copies:
        copy.wait_send()

    def drain(head, carry):
        own_out(head).wait()
        for step in offsets:
            in_copy(head, step).wait_send()
            out_copy(head, step).wait()
        return carry

    lax.fori_loop(0, heads, drain, 0)


def place_kernel(seq_count, span, img, txt, land_ref, gain_ref, *refs):
    outs, sems = refs[:-1], refs[-1]
    copies = [(gain_ref.at[pl.ds(n, 1)], outs[6 + n]) for n in range(2)]
    for j in range(seq_count):
        lanes = pl.ds(j * span, span)
        for kind in range(3):
            copies.append((land_ref.at[j, kind, pl.ds(0, img)], outs[kind].at[0, :, lanes]))
            copies.append((land_ref.at[j, kind, pl.ds(img, txt)], outs[3 + kind].at[0, :, lanes]))
    started = [
        pltpu.make_async_copy(source, target, sems.at[number])
        for number, (source, target) in enumerate(copies)
    ]
    for copy in started:
        copy.start()
    for copy in started:
        copy.wait()


def local(seq_count, iq, ik, iv, idt, tq, tk, tv, td, q_gain, k_gain):
    img, lanes = iq.shape[1], iq.shape[2]
    txt = tq.shape[1]
    rows = img + txt
    heads = lanes // HEAD_DIM // seq_count
    span = heads * HEAD_DIM
    sent = 2 * rows + 2 * img
    peers = seq_count * DP_PARTS[0] - 1 + sum(size - 1 for size in DP_PARTS[1:])
    tokens = [
        pltpu.with_memory_space_constraint(x, pltpu.HBM)
        for x in (iq, ik, iv, idt, tq, tk, tv, td, q_gain[None], k_gain[None])
    ]
    hbm = pl.BlockSpec(memory_space=pltpu.HBM)
    vmem = pl.BlockSpec(memory_space=pltpu.VMEM)
    dma = pltpu.SemaphoreType.DMA
    land, gain = pl.pallas_call(
        functools.partial(exchange_kernel, seq_count, heads, img, txt),
        out_shape=(
            pltpu.VMEM((seq_count, 3, rows, span), BF16),
            pltpu.VMEM((2, HEAD_DIM), F32),
        ),
        in_specs=[hbm] * 10,
        out_specs=(vmem, vmem),
        scratch_shapes=[
            pltpu.VMEM((seq_count, sent, span), BF16),
            pltpu.VMEM((seq_count, heads, sent, HEAD_DIM), BF16),
            pltpu.VMEM((seq_count * txt, span), BF16),
            pltpu.VMEM((seq_count * txt, span), BF16),
            pltpu.VMEM((seq_count, heads, 3, rows, HEAD_DIM), BF16),
            pltpu.VMEM((seq_count, rows, HEAD_DIM), BF16),
            pltpu.VMEM((seq_count, rows, HEAD_DIM), BF16),
            pltpu.VMEM((seq_count * rows, HEAD_DIM), F32),
            pltpu.VMEM((seq_count * rows, HEAD_DIM), F32),
            pltpu.VMEM((len(DP_PARTS), 2, HEAD_DIM), F32),
            pltpu.VMEM((peers, 2, HEAD_DIM), F32),
            dma((seq_count,)),
            dma((4 + heads,)),
            dma((heads, seq_count - 1)),
            dma((heads, seq_count - 1)),
            dma((heads, seq_count - 1)),
            dma((heads, seq_count - 1)),
            dma((heads,)),
            dma((peers,)),
            dma((peers,)),
            pltpu.VMEM((2, HEAD_DIM), F32),
        ],
        compiler_params=pltpu.CompilerParams(collective_id=0, has_side_effects=True, vmem_limit_bytes=40 << 20),
        name="exchange",
    )(*tokens)
    big = jax.ShapeDtypeStruct((1, img, lanes), BF16)
    small = jax.ShapeDtypeStruct((1, txt, lanes), BF16)
    row = jax.ShapeDtypeStruct((1, HEAD_DIM), F32)
    placed = pl.pallas_call(
        functools.partial(place_kernel, seq_count, span, img, txt),
        out_shape=(big,) * 3 + (small,) * 3 + (row,) * 2,
        in_specs=[vmem] * 2,
        out_specs=(hbm,) * 8,
        scratch_shapes=[dma((seq_count * 6 + 2,))],
        compiler_params=pltpu.CompilerParams(vmem_limit_bytes=4 << 20),
        name="place",
    )(*(pltpu.with_memory_space_constraint(x, pltpu.VMEM) for x in (land, gain)))
    return (*placed[:6], placed[6][0], placed[7][0])


def solution(mesh):
    split = P("dp", "seq", None)
    whole = P("dp", None, None)
    return jax.shard_map(
        functools.partial(local, mesh.shape["seq"]),
        mesh=mesh,
        in_specs=(split,) * 5 + (whole,) * 2 + (split, P(), P()),
        out_specs=(split,) * 6 + (P(), P()),
        check_vma=False,
    )
```

```python
import functools

import jax
import jax.numpy as jnp
from jax import lax
from jax.experimental import pallas as pl
from jax.experimental.pallas import tpu as pltpu
from jax.sharding import PartitionSpec as P

HEAD_DIM = 128
EPSILON = 1e-06
HELD = 3
DP_PARTS = (3, 4, 8, 2)
RINGS = (1, 2)
BF16 = jnp.bfloat16
F32 = jnp.float32


def axis_peers(part):
    stride = 1
    for size in DP_PARTS[part + 1 :]:
        stride *= size
    size = DP_PARTS[part]
    index = lax.axis_index("dp")
    place = lax.rem(index // stride, size)
    base = index - place * stride
    return [{"dp": base + lax.rem(place + step, size) * stride} for step in range(1, size)]


def column_peers(seq_count):
    me = lax.axis_index("seq")
    own = [{"dp": lax.axis_index("dp")}] + axis_peers(0)
    return [
        {**lower, "seq": lax.rem(me + step, seq_count)}
        for step in range(seq_count)
        for number, lower in enumerate(own)
        if step or number
    ]


def dot_nt(a, b):
    return lax.dot_general(a, b, (((1,), (1,)), ((), ())), preferred_element_type=F32)


def dot_nn(a, b):
    return lax.dot_general(a, b, (((1,), (0,)), ((), ())), preferred_element_type=F32)


def dot_tn(a, b):
    return lax.dot_general(a, b, (((0,), (0,)), ((), ())), preferred_element_type=F32)


def inverse_rms(x):
    return lax.rsqrt(jnp.mean(x * x, axis=-1, keepdims=True) + EPSILON)


def norm_pull(x, gain, upstream):
    inverse = inverse_rms(x)
    unit = x * inverse
    scaled = upstream * gain
    along = jnp.mean(scaled * unit, axis=-1, keepdims=True)
    return inverse * (scaled - unit * along), upstream * unit


def exchange_kernel(
    seq_count,
    heads,
    img,
    txt,
    iq_ref,
    ik_ref,
    iv_ref,
    id_ref,
    tq_ref,
    tk_ref,
    tv_ref,
    td_ref,
    qg_ref,
    kg_ref,
    land_ref,
    gain_ref,
    stage,
    arrived,
    text_k,
    text_v,
    outgoing,
    keys,
    values,
    key_acc,
    value_acc,
    gain_src,
    gain_in,
    stage_sem,
    own_sem,
    in_send,
    in_recv,
    out_send,
    out_recv,
    own_out_sem,
    gain_send,
    gain_recv,
    gains,
    hello,
):
    me = lax.axis_index("seq")
    rows = img + txt
    span = heads * HEAD_DIM
    scale = HEAD_DIM ** (-0.5)
    offsets = range(1, seq_count)
    seq_peers = [lax.rem(me + step, seq_count) for step in offsets]
    stages = [column_peers(seq_count), axis_peers(3), axis_peers(1), axis_peers(2)]
    near = [(axis_peers(part)[0], axis_peers(part)[-1]) for part in RINGS]
    greeted = column_peers(seq_count) + axis_peers(3) + [peer for pair in near for peer in pair]
    barrier = pltpu.get_barrier_semaphore()
    for peer in greeted:
        pl.semaphore_signal(barrier, inc=1, device_id=peer, device_id_type=pl.DeviceIdType.MESH)

    def fetch(owner, target, sem):
        lanes = pl.ds(pl.multiple_of(owner * span, HEAD_DIM), span)
        row = 0
        for source, count in (
            (iq_ref, img),
            (tq_ref, txt),
            (id_ref, img),
            (td_ref, txt),
            (ik_ref, img),
            (iv_ref, img),
        ):
            pltpu.make_async_copy(
                source.at[0, :, lanes], target.at[pl.ds(row, count), :], sem
            ).start()
            row += count

    for step, peer in zip(offsets, seq_peers):
        fetch(peer, stage.at[step], stage_sem.at[step])
    fetch(me, stage.at[0], stage_sem.at[0])
    my_lanes = pl.ds(pl.multiple_of(me * span, HEAD_DIM), span)
    text_copies = (
        pltpu.make_async_copy(tk_ref.at[0, :, my_lanes], text_k, own_sem.at[0]),
        pltpu.make_async_copy(tv_ref.at[0, :, my_lanes], text_v, own_sem.at[1]),
        pltpu.make_async_copy(qg_ref, gains.at[pl.ds(0, 1)], own_sem.at[2]),
        pltpu.make_async_copy(kg_ref, gains.at[pl.ds(1, 1)], own_sem.at[3]),
    )
    for copy in text_copies:
        copy.start()

    def staged(step):
        return pltpu.make_async_copy(stage.at[step], stage.at[step], stage_sem.at[step])

    for step in offsets:
        staged(step).wait()
    pl.semaphore_wait(barrier, len(greeted))

    def in_copy(head, step):
        lanes = pl.ds(pl.multiple_of(head * HEAD_DIM, HEAD_DIM), HEAD_DIM)
        return pltpu.make_async_remote_copy(
            src_ref=stage.at[step, :, lanes],
            dst_ref=arrived.at[me, head],
            send_sem=in_send.at[head, step - 1],
            recv_sem=in_recv.at[head, step - 1],
            device_id={"seq": lax.rem(me + step, seq_count)},
            device_id_type=pl.DeviceIdType.MESH,
        )

    def out_copy(head, step):
        lanes = pl.ds(pl.multiple_of(head * HEAD_DIM, HEAD_DIM), HEAD_DIM)
        peer = lax.rem(me + step, seq_count)
        return pltpu.make_async_remote_copy(
            src_ref=outgoing.at[peer, head],
            dst_ref=land_ref.at[me, :, :, lanes],
            send_sem=out_send.at[head, step - 1],
            recv_sem=out_recv.at[head, step - 1],
            device_id={"seq": peer},
            device_id_type=pl.DeviceIdType.MESH,
        )

    def own_in(head):
        lanes = pl.ds(pl.multiple_of(head * HEAD_DIM, HEAD_DIM), HEAD_DIM)
        return pltpu.make_async_copy(
            stage.at[0, :, lanes], arrived.at[me, head], own_sem.at[4 + head]
        )

    def own_out(head):
        lanes = pl.ds(pl.multiple_of(head * HEAD_DIM, HEAD_DIM), HEAD_DIM)
        return pltpu.make_async_copy(
            outgoing.at[me, head], land_ref.at[me, :, :, lanes], own_out_sem.at[head]
        )

    def send_out(head):
        for number in range(seq_count - 1):
            peer = number + jnp.where(number >= me, 1, 0)
            out_copy(head, lax.rem(peer - me + seq_count, seq_count)).start()
        own_out(head).start()

    def send_in(head, carry):
        for step in (2, 1, 3):
            in_copy(head, step).start()
        return carry

    lax.fori_loop(0, heads, send_in, 0)
    row = 0
    for pair, part in zip(near, RINGS):
        for _ in range(DP_PARTS[part] // 2 - 1):
            for peer in pair:
                pl.semaphore_signal(
                    hello.at[row], inc=1, device_id=peer, device_id_type=pl.DeviceIdType.MESH
                )
            pl.semaphore_wait(hello.at[row], len(pair))
            row += 1
    staged(0).wait()
    for copy in text_copies:
        copy.wait()

    def move_own(head, carry):
        own_in(head).start()
        return carry

    lax.fori_loop(0, heads, move_own, 0)
    q_gain = gains[0:1]
    k_gain = gains[1:2]
    do_row, k_row, v_row = rows, 2 * rows, 2 * rows + img

    def one_head(head, carry):
        q_total, k_total = carry
        own_in(head).wait()
        for step in offsets:
            in_copy(head, step).wait_recv()
        lanes = pl.ds(pl.multiple_of(head * HEAD_DIM, HEAD_DIM), HEAD_DIM)

        def raw_keys(j):
            return jnp.concatenate(
                [
                    arrived[j, head, k_row : k_row + img, :].astype(F32),
                    text_k[j * txt : (j + 1) * txt, lanes].astype(F32),
                ],
                axis=0,
            )

        for j in range(seq_count):
            x = raw_keys(j)
            keys[j] = (x * inverse_rms(x) * k_gain).astype(BF16)
            values[j, :img] = arrived[j, head, v_row : v_row + img, :]
            values[j, img:] = text_v[j * txt : (j + 1) * txt, lanes]
        kn = keys[...].reshape(seq_count * rows, HEAD_DIM)
        vv = values[...].reshape(seq_count * rows, HEAD_DIM)
        for j in range(seq_count):
            xq = arrived[j, head, :rows, :].astype(F32)
            qn = (xq * inverse_rms(xq) * q_gain).astype(BF16)
            dout = arrived[j, head, do_row : do_row + rows, :]
            scores = dot_nt(qn, kn) * scale
            weights = jnp.exp(scores - jnp.max(scores, axis=-1, keepdims=True))
            prob = weights * (1.0 / jnp.sum(weights, axis=-1, keepdims=True))
            prob_b = prob.astype(BF16)
            out_b = dot_nn(prob_b, vv).astype(BF16)
            delta = jnp.sum(dout.astype(F32) * out_b.astype(F32), axis=-1, keepdims=True)
            dscore = (prob * (dot_nt(dout, vv) - delta) * scale).astype(BF16)
            dq = dot_nn(dscore, kn)
            key_part = dot_tn(dscore, qn).astype(BF16).astype(F32)
            value_part = dot_tn(prob_b, dout).astype(BF16).astype(F32)
            if j == 0:
                key_acc[...] = key_part
                value_acc[...] = value_part
            else:
                key_acc[...] += key_part
                value_acc[...] += value_part
            dx, terms = norm_pull(xq, q_gain, dq)
            outgoing[j, head, 0] = dx.astype(BF16)
            q_total += jnp.sum(terms, axis=0, keepdims=True)
        for j in range(seq_count):
            dx, terms = norm_pull(raw_keys(j), k_gain, key_acc[j * rows : (j + 1) * rows])
            outgoing[j, head, 1] = dx.astype(BF16)
            outgoing[j, head, 2] = value_acc[j * rows : (j + 1) * rows].astype(BF16)
            k_total += jnp.sum(terms, axis=0, keepdims=True)

        @pl.when(head < heads - HELD)
        def _():
            send_out(head)

        return q_total, k_total

    zero = jnp.zeros((1, HEAD_DIM), F32)
    q_total, k_total = lax.fori_loop(0, heads, one_head, (zero, zero))
    gain = jnp.concatenate([q_total, k_total], axis=0)
    slot = 0
    copies = []
    for number, peers in enumerate(stages):
        gain_src[number] = gain
        current = []
        for index, peer in enumerate(peers):
            copy = pltpu.make_async_remote_copy(
                src_ref=gain_src.at[number],
                dst_ref=gain_in.at[slot + index],
                send_sem=gain_send.at[slot + index],
                recv_sem=gain_recv.at[slot + index],
                device_id=peer,
                device_id_type=pl.DeviceIdType.MESH,
            )
            copy.start()
            current.append(copy)
        if number == 0:
            for head in range(heads - HELD, heads):
                send_out(head)
        for index, copy in enumerate(current):
            copy.wait_recv()
            gain = gain + gain_in[slot + index]
        copies += current
        slot += len(peers)
    gain_ref[...] = gain
    for copy in copies:
        copy.wait_send()

    def drain(head, carry):
        own_out(head).wait()
        for step in offsets:
            in_copy(head, step).wait_send()
            out_copy(head, step).wait()
        return carry

    lax.fori_loop(0, heads, drain, 0)


def place_kernel(seq_count, span, img, txt, land_ref, gain_ref, *refs):
    outs, sems = refs[:-1], refs[-1]
    copies = [(gain_ref.at[pl.ds(n, 1)], outs[6 + n]) for n in range(2)]
    for j in range(seq_count):
        lanes = pl.ds(j * span, span)
        for kind in range(3):
            copies.append((land_ref.at[j, kind, pl.ds(0, img)], outs[kind].at[0, :, lanes]))
            copies.append((land_ref.at[j, kind, pl.ds(img, txt)], outs[3 + kind].at[0, :, lanes]))
    started = [
        pltpu.make_async_copy(source, target, sems.at[number])
        for number, (source, target) in enumerate(copies)
    ]
    for copy in started:
        copy.start()
    for copy in started:
        copy.wait()


def local(seq_count, iq, ik, iv, idt, tq, tk, tv, td, q_gain, k_gain):
    img, lanes = iq.shape[1], iq.shape[2]
    txt = tq.shape[1]
    rows = img + txt
    heads = lanes // HEAD_DIM // seq_count
    span = heads * HEAD_DIM
    sent = 2 * rows + 2 * img
    peers = seq_count * DP_PARTS[0] - 1 + sum(size - 1 for size in DP_PARTS[1:])
    tokens = [
        pltpu.with_memory_space_constraint(x, pltpu.HBM)
        for x in (iq, ik, iv, idt, tq, tk, tv, td, q_gain[None], k_gain[None])
    ]
    hbm = pl.BlockSpec(memory_space=pltpu.HBM)
    vmem = pl.BlockSpec(memory_space=pltpu.VMEM)
    dma = pltpu.SemaphoreType.DMA
    land, gain = pl.pallas_call(
        functools.partial(exchange_kernel, seq_count, heads, img, txt),
        out_shape=(
            pltpu.VMEM((seq_count, 3, rows, span), BF16),
            pltpu.VMEM((2, HEAD_DIM), F32),
        ),
        in_specs=[hbm] * 10,
        out_specs=(vmem, vmem),
        scratch_shapes=[
            pltpu.VMEM((seq_count, sent, span), BF16),
            pltpu.VMEM((seq_count, heads, sent, HEAD_DIM), BF16),
            pltpu.VMEM((seq_count * txt, span), BF16),
            pltpu.VMEM((seq_count * txt, span), BF16),
            pltpu.VMEM((seq_count, heads, 3, rows, HEAD_DIM), BF16),
            pltpu.VMEM((seq_count, rows, HEAD_DIM), BF16),
            pltpu.VMEM((seq_count, rows, HEAD_DIM), BF16),
            pltpu.VMEM((seq_count * rows, HEAD_DIM), F32),
            pltpu.VMEM((seq_count * rows, HEAD_DIM), F32),
            pltpu.VMEM((len(DP_PARTS), 2, HEAD_DIM), F32),
            pltpu.VMEM((peers, 2, HEAD_DIM), F32),
            dma((seq_count,)),
            dma((4 + heads,)),
            dma((heads, seq_count - 1)),
            dma((heads, seq_count - 1)),
            dma((heads, seq_count - 1)),
            dma((heads, seq_count - 1)),
            dma((heads,)),
            dma((peers,)),
            dma((peers,)),
            pltpu.VMEM((2, HEAD_DIM), F32),
            pltpu.SemaphoreType.REGULAR((sum(DP_PARTS[part] // 2 - 1 for part in RINGS),)),
        ],
        compiler_params=pltpu.CompilerParams(collective_id=0, has_side_effects=True, vmem_limit_bytes=40 << 20),
        name="exchange",
    )(*tokens)
    big = jax.ShapeDtypeStruct((1, img, lanes), BF16)
    small = jax.ShapeDtypeStruct((1, txt, lanes), BF16)
    row = jax.ShapeDtypeStruct((1, HEAD_DIM), F32)
    placed = pl.pallas_call(
        functools.partial(place_kernel, seq_count, span, img, txt),
        out_shape=(big,) * 3 + (small,) * 3 + (row,) * 2,
        in_specs=[vmem] * 2,
        out_specs=(hbm,) * 8,
        scratch_shapes=[dma((seq_count * 6 + 2,))],
        compiler_params=pltpu.CompilerParams(vmem_limit_bytes=4 << 20),
        name="place",
    )(*(pltpu.with_memory_space_constraint(x, pltpu.VMEM) for x in (land, gain)))
    return (*placed[:6], placed[6][0], placed[7][0])


def solution(mesh):
    split = P("dp", "seq", None)
    whole = P("dp", None, None)
    return jax.shard_map(
        functools.partial(local, mesh.shape["seq"]),
        mesh=mesh,
        in_specs=(split,) * 5 + (whole,) * 2 + (split, P(), P()),
        out_specs=(split,) * 6 + (P(), P()),
        check_vma=False,
    )
```

```python
import functools

import jax
import jax.numpy as jnp
from jax import lax
from jax.experimental import pallas as pl
from jax.experimental.pallas import tpu as pltpu
from jax.sharding import PartitionSpec as P

HEAD_DIM = 128
EPSILON = 1e-06
LOG2E = 1.4426950408889634
HELD = 3
DP_PARTS = (3, 4, 8, 2)
RINGS = (1, 2)
BF16 = jnp.bfloat16
F32 = jnp.float32


def axis_peers(part):
    stride = 1
    for size in DP_PARTS[part + 1 :]:
        stride *= size
    size = DP_PARTS[part]
    index = lax.axis_index("dp")
    place = lax.rem(index // stride, size)
    base = index - place * stride
    return [{"dp": base + lax.rem(place + step, size) * stride} for step in range(1, size)]


def column_peers(seq_count):
    me = lax.axis_index("seq")
    own = [{"dp": lax.axis_index("dp")}] + axis_peers(0)
    return [
        {**lower, "seq": lax.rem(me + step, seq_count)}
        for step in range(seq_count)
        for number, lower in enumerate(own)
        if step or number
    ]


def dot_nt(a, b):
    return lax.dot_general(a, b, (((1,), (1,)), ((), ())), preferred_element_type=F32)


def dot_nn(a, b):
    return lax.dot_general(a, b, (((1,), (0,)), ((), ())), preferred_element_type=F32)


def dot_tn(a, b):
    return lax.dot_general(a, b, (((0,), (0,)), ((), ())), preferred_element_type=F32)


def inverse_rms(x):
    return lax.rsqrt(jnp.mean(x * x, axis=-1, keepdims=True) + EPSILON)


def norm_pull(x, gain, upstream):
    inverse = inverse_rms(x)
    unit = x * inverse
    scaled = upstream * gain
    along = jnp.mean(scaled * unit, axis=-1, keepdims=True)
    return inverse * (scaled - unit * along), upstream * unit


def exchange_kernel(
    seq_count,
    heads,
    img,
    txt,
    iq_ref,
    ik_ref,
    iv_ref,
    id_ref,
    tq_ref,
    tk_ref,
    tv_ref,
    td_ref,
    qg_ref,
    kg_ref,
    land_ref,
    gain_ref,
    stage,
    arrived,
    text_k,
    text_v,
    outgoing,
    keys,
    values,
    key_acc,
    value_acc,
    gain_src,
    gain_in,
    stage_sem,
    own_sem,
    in_send,
    in_recv,
    out_send,
    out_recv,
    own_out_sem,
    gain_send,
    gain_recv,
    gains,
    hello,
):
    me = lax.axis_index("seq")
    rows = img + txt
    span = heads * HEAD_DIM
    scale = HEAD_DIM ** (-0.5)
    offsets = range(1, seq_count)
    seq_peers = [lax.rem(me + step, seq_count) for step in offsets]
    stages = [column_peers(seq_count), axis_peers(3), axis_peers(1), axis_peers(2)]
    near = [(axis_peers(part)[0], axis_peers(part)[-1]) for part in RINGS]
    greeted = column_peers(seq_count) + axis_peers(3) + [peer for pair in near for peer in pair]
    barrier = pltpu.get_barrier_semaphore()
    def fetch(owner, target, sem):
        lanes = pl.ds(pl.multiple_of(owner * span, HEAD_DIM), span)
        row = 0
        for source, count in (
            (iq_ref, img),
            (tq_ref, txt),
            (id_ref, img),
            (td_ref, txt),
            (ik_ref, img),
            (iv_ref, img),
        ):
            pltpu.make_async_copy(
                source.at[0, :, lanes], target.at[pl.ds(row, count), :], sem
            ).start()
            row += count

    for step in (2, 1, 3):
        fetch(seq_peers[step - 1], stage.at[step], stage_sem.at[step])
    for peer in greeted:
        pl.semaphore_signal(barrier, inc=1, device_id=peer, device_id_type=pl.DeviceIdType.MESH)
    fetch(me, stage.at[0], stage_sem.at[0])
    my_lanes = pl.ds(pl.multiple_of(me * span, HEAD_DIM), span)
    text_copies = (
        pltpu.make_async_copy(tk_ref.at[0, :, my_lanes], text_k, own_sem.at[0]),
        pltpu.make_async_copy(tv_ref.at[0, :, my_lanes], text_v, own_sem.at[1]),
        pltpu.make_async_copy(qg_ref, gains.at[pl.ds(0, 1)], own_sem.at[2]),
        pltpu.make_async_copy(kg_ref, gains.at[pl.ds(1, 1)], own_sem.at[3]),
    )
    for copy in text_copies:
        copy.start()

    def staged(step):
        return pltpu.make_async_copy(stage.at[step], stage.at[step], stage_sem.at[step])

    for step in offsets:
        staged(step).wait()
    pl.semaphore_wait(barrier, len(greeted))

    def in_copy(head, step):
        lanes = pl.ds(pl.multiple_of(head * HEAD_DIM, HEAD_DIM), HEAD_DIM)
        return pltpu.make_async_remote_copy(
            src_ref=stage.at[step, :, lanes],
            dst_ref=arrived.at[me, head],
            send_sem=in_send.at[head, step - 1],
            recv_sem=in_recv.at[head, step - 1],
            device_id={"seq": lax.rem(me + step, seq_count)},
            device_id_type=pl.DeviceIdType.MESH,
        )

    def out_copy(head, step):
        lanes = pl.ds(pl.multiple_of(head * HEAD_DIM, HEAD_DIM), HEAD_DIM)
        peer = lax.rem(me + step, seq_count)
        return pltpu.make_async_remote_copy(
            src_ref=outgoing.at[peer, head],
            dst_ref=land_ref.at[me, :, :, lanes],
            send_sem=out_send.at[head, step - 1],
            recv_sem=out_recv.at[head, step - 1],
            device_id={"seq": peer},
            device_id_type=pl.DeviceIdType.MESH,
        )

    def own_in(head):
        lanes = pl.ds(pl.multiple_of(head * HEAD_DIM, HEAD_DIM), HEAD_DIM)
        return pltpu.make_async_copy(
            stage.at[0, :, lanes], arrived.at[me, head], own_sem.at[4 + head]
        )

    def own_out(head):
        lanes = pl.ds(pl.multiple_of(head * HEAD_DIM, HEAD_DIM), HEAD_DIM)
        return pltpu.make_async_copy(
            outgoing.at[me, head], land_ref.at[me, :, :, lanes], own_out_sem.at[head]
        )

    def send_out(head):
        for number in range(seq_count - 1):
            peer = number + jnp.where(number >= me, 1, 0)
            out_copy(head, lax.rem(peer - me + seq_count, seq_count)).start()
        own_out(head).start()

    def send_in(head, carry):
        for step in (2, 1, 3):
            in_copy(head, step).start()
        return carry

    lax.fori_loop(0, heads, send_in, 0)
    row = 0
    for pair, part in zip(near, RINGS):
        for _ in range(DP_PARTS[part] // 2 - 1):
            for peer in pair:
                pl.semaphore_signal(
                    hello.at[row], inc=1, device_id=peer, device_id_type=pl.DeviceIdType.MESH
                )
            pl.semaphore_wait(hello.at[row], len(pair))
            row += 1
    staged(0).wait()
    for copy in text_copies:
        copy.wait()

    def move_own(head, carry):
        own_in(head).start()
        return carry

    lax.fori_loop(0, heads, move_own, 0)
    q_gain = gains[0:1]
    k_gain = gains[1:2]
    do_row, k_row, v_row = rows, 2 * rows, 2 * rows + img

    def one_head(head, carry):
        q_total, k_total = carry
        own_in(head).wait()
        for step in offsets:
            in_copy(head, step).wait_recv()
        lanes = pl.ds(pl.multiple_of(head * HEAD_DIM, HEAD_DIM), HEAD_DIM)

        def raw_keys(j):
            return jnp.concatenate(
                [
                    arrived[j, head, k_row : k_row + img, :].astype(F32),
                    text_k[j * txt : (j + 1) * txt, lanes].astype(F32),
                ],
                axis=0,
            )

        for j in range(seq_count):
            x = raw_keys(j)
            keys[j] = (x * inverse_rms(x) * k_gain).astype(BF16)
            values[j, :img] = arrived[j, head, v_row : v_row + img, :]
            values[j, img:] = text_v[j * txt : (j + 1) * txt, lanes]
        kn = keys[...].reshape(seq_count * rows, HEAD_DIM)
        vv = values[...].reshape(seq_count * rows, HEAD_DIM)
        def first_dots(j):
            xq = arrived[j, head, :rows, :].astype(F32)
            qn = (xq * inverse_rms(xq) * q_gain).astype(BF16)
            dout = arrived[j, head, do_row : do_row + rows, :]
            return qn, dot_nt(qn, kn), dot_nt(dout, vv)

        def soften(scores):
            weights = jnp.exp2((scores - jnp.max(scores, axis=-1, keepdims=True)) * (scale * LOG2E))
            prob = weights * (1.0 / jnp.sum(weights, axis=-1, keepdims=True))
            return prob, prob.astype(BF16)

        def score_gradient(j, prob, prob_b, dprob):
            dout = arrived[j, head, do_row : do_row + rows, :]
            out_b = dot_nn(prob_b, vv).astype(BF16)
            delta = jnp.sum(dout.astype(F32) * out_b.astype(F32), axis=-1, keepdims=True)
            return (prob * (dprob - delta) * scale).astype(BF16)

        def value_terms(j, prob_b):
            dout = arrived[j, head, do_row : do_row + rows, :]
            value_part = dot_tn(prob_b, dout).astype(BF16).astype(F32)
            value_acc[...] = value_part if j == 0 else value_acc[...] + value_part

        def last_dots(j, qn, dscore):
            key_part = dot_tn(dscore, qn).astype(BF16).astype(F32)
            key_acc[...] = key_part if j == 0 else key_acc[...] + key_part
            xq = arrived[j, head, :rows, :].astype(F32)
            dx, terms = norm_pull(xq, q_gain, dot_nn(dscore, kn))
            outgoing[j, head, 0] = dx.astype(BF16)
            return jnp.sum(terms, axis=0, keepdims=True)

        blocks, softs, dscores = {}, {}, {}
        for step, j in (("first", 0), ("soft", 0), ("first", 1), ("score", 0), ("value", 0), ("soft", 1), ("first", 2), ("last", 0), ("score", 1), ("value", 1), ("soft", 2), ("first", 3), ("last", 1), ("score", 2), ("value", 2), ("soft", 3), ("last", 2), ("score", 3), ("value", 3), ("last", 3)):
            if step == "first":
                blocks[j] = first_dots(j)
            elif step == "soft":
                softs[j] = soften(blocks[j][1])
            elif step == "score":
                dscores[j] = score_gradient(j, *softs[j], blocks[j][2])
            elif step == "value":
                value_terms(j, softs[j][1])
            else:
                q_total += last_dots(j, blocks[j][0], dscores[j])
        for j in range(seq_count):
            dx, terms = norm_pull(raw_keys(j), k_gain, key_acc[j * rows : (j + 1) * rows])
            outgoing[j, head, 1] = dx.astype(BF16)
            outgoing[j, head, 2] = value_acc[j * rows : (j + 1) * rows].astype(BF16)
            k_total += jnp.sum(terms, axis=0, keepdims=True)

        @pl.when(head < heads - HELD)
        def _():
            send_out(head)

        return q_total, k_total

    zero = jnp.zeros((1, HEAD_DIM), F32)
    q_total, k_total = lax.fori_loop(0, heads, one_head, (zero, zero))
    gain = jnp.concatenate([q_total, k_total], axis=0)
    slot = 0
    copies = []
    for number, peers in enumerate(stages):
        gain_src[number] = gain
        current = []
        for index, peer in enumerate(peers):
            copy = pltpu.make_async_remote_copy(
                src_ref=gain_src.at[number],
                dst_ref=gain_in.at[slot + index],
                send_sem=gain_send.at[slot + index],
                recv_sem=gain_recv.at[slot + index],
                device_id=peer,
                device_id_type=pl.DeviceIdType.MESH,
            )
            copy.start()
            current.append(copy)
        if number == 0:
            for head in range(heads - HELD, heads):
                send_out(head)
        for index, copy in enumerate(current):
            copy.wait_recv()
            gain = gain + gain_in[slot + index]
        copies += current
        slot += len(peers)
    gain_ref[...] = gain
    for copy in copies:
        copy.wait_send()

    def drain(head, carry):
        own_out(head).wait()
        for step in offsets:
            in_copy(head, step).wait_send()
            out_copy(head, step).wait()
        return carry

    lax.fori_loop(0, heads, drain, 0)


def place_kernel(seq_count, span, img, txt, land_ref, gain_ref, *refs):
    outs, sems = refs[:-1], refs[-1]
    copies = [(gain_ref.at[pl.ds(n, 1)], outs[6 + n]) for n in range(2)]
    for j in range(seq_count):
        lanes = pl.ds(j * span, span)
        for kind in range(3):
            copies.append((land_ref.at[j, kind, pl.ds(0, img)], outs[kind].at[0, :, lanes]))
            copies.append((land_ref.at[j, kind, pl.ds(img, txt)], outs[3 + kind].at[0, :, lanes]))
    started = [
        pltpu.make_async_copy(source, target, sems.at[number])
        for number, (source, target) in enumerate(copies)
    ]
    for copy in started:
        copy.start()
    for copy in started:
        copy.wait()


def local(seq_count, iq, ik, iv, idt, tq, tk, tv, td, q_gain, k_gain):
    img, lanes = iq.shape[1], iq.shape[2]
    txt = tq.shape[1]
    rows = img + txt
    heads = lanes // HEAD_DIM // seq_count
    span = heads * HEAD_DIM
    sent = 2 * rows + 2 * img
    peers = seq_count * DP_PARTS[0] - 1 + sum(size - 1 for size in DP_PARTS[1:])
    tokens = [
        pltpu.with_memory_space_constraint(x, pltpu.HBM)
        for x in (iq, ik, iv, idt, tq, tk, tv, td, q_gain[None], k_gain[None])
    ]
    hbm = pl.BlockSpec(memory_space=pltpu.HBM)
    vmem = pl.BlockSpec(memory_space=pltpu.VMEM)
    dma = pltpu.SemaphoreType.DMA
    land, gain = pl.pallas_call(
        functools.partial(exchange_kernel, seq_count, heads, img, txt),
        out_shape=(
            pltpu.VMEM((seq_count, 3, rows, span), BF16),
            pltpu.VMEM((2, HEAD_DIM), F32),
        ),
        in_specs=[hbm] * 10,
        out_specs=(vmem, vmem),
        scratch_shapes=[
            pltpu.VMEM((seq_count, sent, span), BF16),
            pltpu.VMEM((seq_count, heads, sent, HEAD_DIM), BF16),
            pltpu.VMEM((seq_count * txt, span), BF16),
            pltpu.VMEM((seq_count * txt, span), BF16),
            pltpu.VMEM((seq_count, heads, 3, rows, HEAD_DIM), BF16),
            pltpu.VMEM((seq_count, rows, HEAD_DIM), BF16),
            pltpu.VMEM((seq_count, rows, HEAD_DIM), BF16),
            pltpu.VMEM((seq_count * rows, HEAD_DIM), F32),
            pltpu.VMEM((seq_count * rows, HEAD_DIM), F32),
            pltpu.VMEM((len(DP_PARTS), 2, HEAD_DIM), F32),
            pltpu.VMEM((peers, 2, HEAD_DIM), F32),
            dma((seq_count,)),
            dma((4 + heads,)),
            dma((heads, seq_count - 1)),
            dma((heads, seq_count - 1)),
            dma((heads, seq_count - 1)),
            dma((heads, seq_count - 1)),
            dma((heads,)),
            dma((peers,)),
            dma((peers,)),
            pltpu.VMEM((2, HEAD_DIM), F32),
            pltpu.SemaphoreType.REGULAR((sum(DP_PARTS[part] // 2 - 1 for part in RINGS),)),
        ],
        compiler_params=pltpu.CompilerParams(collective_id=0, has_side_effects=True, vmem_limit_bytes=40 << 20),
        name="exchange",
    )(*tokens)
    big = jax.ShapeDtypeStruct((1, img, lanes), BF16)
    small = jax.ShapeDtypeStruct((1, txt, lanes), BF16)
    row = jax.ShapeDtypeStruct((1, HEAD_DIM), F32)
    placed = pl.pallas_call(
        functools.partial(place_kernel, seq_count, span, img, txt),
        out_shape=(big,) * 3 + (small,) * 3 + (row,) * 2,
        in_specs=[vmem] * 2,
        out_specs=(hbm,) * 8,
        scratch_shapes=[dma((seq_count * 6 + 2,))],
        compiler_params=pltpu.CompilerParams(vmem_limit_bytes=4 << 20),
        name="place",
    )(*(pltpu.with_memory_space_constraint(x, pltpu.VMEM) for x in (land, gain)))
    return (*placed[:6], placed[6][0], placed[7][0])


def solution(mesh):
    split = P("dp", "seq", None)
    whole = P("dp", None, None)
    return jax.shard_map(
        functools.partial(local, mesh.shape["seq"]),
        mesh=mesh,
        in_specs=(split,) * 5 + (whole,) * 2 + (split, P(), P()),
        out_specs=(split,) * 6 + (P(), P()),
        check_vma=False,
    )
```

```python
import functools

import jax
import jax.numpy as jnp
from jax import lax
from jax.experimental import pallas as pl
from jax.experimental.pallas import tpu as pltpu
from jax.sharding import PartitionSpec as P

HEAD_DIM = 128
EPSILON = 1e-06
LOG2E = 1.4426950408889634
HELD = 3
DP_PARTS = (3, 4, 8, 2)
RINGS = (1, 2)
BF16 = jnp.bfloat16
F32 = jnp.float32


def axis_peers(part):
    stride = 1
    for size in DP_PARTS[part + 1 :]:
        stride *= size
    size = DP_PARTS[part]
    index = lax.axis_index("dp")
    place = lax.rem(index // stride, size)
    base = index - place * stride
    return [{"dp": base + lax.rem(place + step, size) * stride} for step in range(1, size)]


def column_peers(seq_count):
    me = lax.axis_index("seq")
    own = [{"dp": lax.axis_index("dp")}] + axis_peers(0)
    return [
        {**lower, "seq": lax.rem(me + step, seq_count)}
        for step in range(seq_count)
        for number, lower in enumerate(own)
        if step or number
    ]


def dot_nt(a, b):
    return lax.dot_general(a, b, (((1,), (1,)), ((), ())), preferred_element_type=F32)


def dot_nn(a, b):
    return lax.dot_general(a, b, (((1,), (0,)), ((), ())), preferred_element_type=F32)


def dot_tn(a, b):
    return lax.dot_general(a, b, (((0,), (0,)), ((), ())), preferred_element_type=F32)


def inverse_rms(x):
    return lax.rsqrt(jnp.mean(x * x, axis=-1, keepdims=True) + EPSILON)


def norm_pull(x, gain, upstream):
    inverse = inverse_rms(x)
    unit = x * inverse
    scaled = upstream * gain
    along = jnp.mean(scaled * unit, axis=-1, keepdims=True)
    return inverse * (scaled - unit * along), upstream * unit


def wait_bytes(ref, sem):
    pltpu.make_async_copy(ref, ref, sem).wait()


def exchange_kernel(
    seq_count,
    heads,
    img,
    txt,
    iq_ref,
    ik_ref,
    iv_ref,
    id_ref,
    tq_ref,
    tk_ref,
    tv_ref,
    td_ref,
    qg_ref,
    kg_ref,
    land_ref,
    gain_ref,
    stage,
    arrived,
    text_k,
    text_v,
    outgoing,
    keys,
    values,
    key_acc,
    value_acc,
    gain_src,
    gain_in,
    stage_sem,
    own_sem,
    in_send,
    in_recv,
    out_send,
    out_recv,
    own_out_sem,
    gain_send,
    gain_recv,
    gains,
    hello,
):
    me = lax.axis_index("seq")
    rows = img + txt
    span = heads * HEAD_DIM
    scale = HEAD_DIM ** (-0.5)
    offsets = range(1, seq_count)
    seq_peers = [lax.rem(me + step, seq_count) for step in offsets]
    stages = [column_peers(seq_count), axis_peers(3), axis_peers(1), axis_peers(2)]
    near = [(axis_peers(part)[0], axis_peers(part)[-1]) for part in RINGS]
    greeted = column_peers(seq_count) + axis_peers(3) + [peer for pair in near for peer in pair]
    barrier = pltpu.get_barrier_semaphore()
    def fetch(owner, target, sem):
        lanes = pl.ds(pl.multiple_of(owner * span, HEAD_DIM), span)
        row = 0
        for source, count in (
            (iq_ref, img),
            (tq_ref, txt),
            (id_ref, img),
            (td_ref, txt),
            (ik_ref, img),
            (iv_ref, img),
        ):
            pltpu.make_async_copy(
                source.at[0, :, lanes], target.at[pl.ds(row, count), :], sem
            ).start()
            row += count

    for step in (2, 1, 3):
        fetch(seq_peers[step - 1], stage.at[step], stage_sem.at[step])
    for peer in greeted:
        pl.semaphore_signal(barrier, inc=1, device_id=peer, device_id_type=pl.DeviceIdType.MESH)
    def in_copy(head, step):
        lanes = pl.ds(pl.multiple_of(head * HEAD_DIM, HEAD_DIM), HEAD_DIM)
        return pltpu.make_async_remote_copy(
            src_ref=stage.at[step, :, lanes],
            dst_ref=arrived.at[me, head],
            send_sem=in_send.at[0],
            recv_sem=in_recv.at[head],
            device_id={"seq": lax.rem(me + step, seq_count)},
            device_id_type=pl.DeviceIdType.MESH,
        )

    def out_copy(head, step):
        lanes = pl.ds(pl.multiple_of(head * HEAD_DIM, HEAD_DIM), HEAD_DIM)
        peer = lax.rem(me + step, seq_count)
        return pltpu.make_async_remote_copy(
            src_ref=outgoing.at[peer, head],
            dst_ref=land_ref.at[me, :, :, lanes],
            send_sem=out_send.at[0],
            recv_sem=out_recv.at[0],
            device_id={"seq": peer},
            device_id_type=pl.DeviceIdType.MESH,
        )

    def own_in(head):
        lanes = pl.ds(pl.multiple_of(head * HEAD_DIM, HEAD_DIM), HEAD_DIM)
        return pltpu.make_async_copy(
            stage.at[0, :, lanes], arrived.at[me, head], own_sem.at[4 + head]
        )

    def own_out(head):
        lanes = pl.ds(pl.multiple_of(head * HEAD_DIM, HEAD_DIM), HEAD_DIM)
        return pltpu.make_async_copy(
            outgoing.at[me, head], land_ref.at[me, :, :, lanes], own_out_sem.at[0]
        )

    def send_out(head):
        for number in range(seq_count - 1):
            peer = number + jnp.where(number >= me, 1, 0)
            out_copy(head, lax.rem(peer - me + seq_count, seq_count)).start()
        own_out(head).start()

    def send_in(head, carry):
        for step in (2, 1, 3):
            in_copy(head, step).start()
        return carry

    def staged(step):
        wait_bytes(stage.at[step], stage_sem.at[step])

    staged(2)
    pl.semaphore_wait(barrier, len(greeted))
    in_copy(0, 2).start()
    for step in (1, 3):
        staged(step)
        in_copy(0, step).start()
    lax.fori_loop(1, heads, send_in, 0)
    fetch(me, stage.at[0], stage_sem.at[0])
    my_lanes = pl.ds(pl.multiple_of(me * span, HEAD_DIM), span)
    text_copies = (
        pltpu.make_async_copy(tk_ref.at[0, :, my_lanes], text_k, own_sem.at[0]),
        pltpu.make_async_copy(tv_ref.at[0, :, my_lanes], text_v, own_sem.at[1]),
        pltpu.make_async_copy(qg_ref, gains.at[pl.ds(0, 1)], own_sem.at[2]),
        pltpu.make_async_copy(kg_ref, gains.at[pl.ds(1, 1)], own_sem.at[3]),
    )
    for copy in text_copies:
        copy.start()

    row = 0
    for pair, part in zip(near, RINGS):
        for _ in range(DP_PARTS[part] // 2 - 1):
            for peer in pair:
                pl.semaphore_signal(
                    hello.at[row], inc=1, device_id=peer, device_id_type=pl.DeviceIdType.MESH
                )
            pl.semaphore_wait(hello.at[row], len(pair))
            row += 1
    staged(0)
    for copy in text_copies:
        copy.wait()

    def move_own(head, carry):
        own_in(head).start()
        return carry

    lax.fori_loop(0, heads, move_own, 0)
    q_gain = gains[0:1]
    k_gain = gains[1:2]
    do_row, k_row, v_row = rows, 2 * rows, 2 * rows + img

    def one_head(head, carry):
        q_total, k_total = carry
        own_in(head).wait()
        wait_bytes(arrived.at[pl.ds(0, seq_count - 1), head], in_recv.at[head])
        lanes = pl.ds(pl.multiple_of(head * HEAD_DIM, HEAD_DIM), HEAD_DIM)

        def raw_keys(j):
            return jnp.concatenate(
                [
                    arrived[j, head, k_row : k_row + img, :].astype(F32),
                    text_k[j * txt : (j + 1) * txt, lanes].astype(F32),
                ],
                axis=0,
            )

        for j in range(seq_count):
            x = raw_keys(j)
            keys[j] = (x * inverse_rms(x) * k_gain).astype(BF16)
            values[j, :img] = arrived[j, head, v_row : v_row + img, :]
            values[j, img:] = text_v[j * txt : (j + 1) * txt, lanes]
        kn = keys[...].reshape(seq_count * rows, HEAD_DIM)
        vv = values[...].reshape(seq_count * rows, HEAD_DIM)
        def first_dots(j):
            xq = arrived[j, head, :rows, :].astype(F32)
            qn = (xq * inverse_rms(xq) * q_gain).astype(BF16)
            dout = arrived[j, head, do_row : do_row + rows, :]
            return qn, dot_nt(qn, kn), dot_nt(dout, vv)

        def soften(scores):
            weights = jnp.exp2((scores - jnp.max(scores, axis=-1, keepdims=True)) * (scale * LOG2E))
            prob = weights * (1.0 / jnp.sum(weights, axis=-1, keepdims=True))
            return prob, prob.astype(BF16)

        def score_gradient(j, prob, prob_b, dprob):
            dout = arrived[j, head, do_row : do_row + rows, :]
            out_b = dot_nn(prob_b, vv).astype(BF16)
            delta = jnp.sum(dout.astype(F32) * out_b.astype(F32), axis=-1, keepdims=True)
            return (prob * (dprob - delta) * scale).astype(BF16)

        def value_terms(j, prob_b):
            dout = arrived[j, head, do_row : do_row + rows, :]
            value_part = dot_tn(prob_b, dout).astype(BF16).astype(F32)
            value_acc[...] = value_part if j == 0 else value_acc[...] + value_part

        def last_dots(j, qn, dscore):
            key_part = dot_tn(dscore, qn).astype(BF16).astype(F32)
            key_acc[...] = key_part if j == 0 else key_acc[...] + key_part
            xq = arrived[j, head, :rows, :].astype(F32)
            dx, terms = norm_pull(xq, q_gain, dot_nn(dscore, kn))
            outgoing[j, head, 0] = dx.astype(BF16)
            return jnp.sum(terms, axis=0, keepdims=True)

        blocks, softs, dscores = {}, {}, {}
        for step, j in (("first", 0), ("soft", 0), ("first", 1), ("score", 0), ("value", 0), ("soft", 1), ("first", 2), ("last", 0), ("score", 1), ("value", 1), ("soft", 2), ("first", 3), ("last", 1), ("score", 2), ("value", 2), ("soft", 3), ("last", 2), ("score", 3), ("value", 3), ("last", 3)):
            if step == "first":
                blocks[j] = first_dots(j)
            elif step == "soft":
                softs[j] = soften(blocks[j][1])
            elif step == "score":
                dscores[j] = score_gradient(j, *softs[j], blocks[j][2])
            elif step == "value":
                value_terms(j, softs[j][1])
            else:
                q_total += last_dots(j, blocks[j][0], dscores[j])
        for j in range(seq_count):
            dx, terms = norm_pull(raw_keys(j), k_gain, key_acc[j * rows : (j + 1) * rows])
            outgoing[j, head, 1] = dx.astype(BF16)
            outgoing[j, head, 2] = value_acc[j * rows : (j + 1) * rows].astype(BF16)
            k_total += jnp.sum(terms, axis=0, keepdims=True)

        @pl.when(head < heads - HELD)
        def _():
            send_out(head)

        return q_total, k_total

    zero = jnp.zeros((1, HEAD_DIM), F32)
    q_total, k_total = lax.fori_loop(0, heads, one_head, (zero, zero))
    gain = jnp.concatenate([q_total, k_total], axis=0)
    slot = 0
    for number, peers in enumerate(stages):
        gain_src[number] = gain
        for index, peer in enumerate(peers):
            copy = pltpu.make_async_remote_copy(
                src_ref=gain_src.at[number],
                dst_ref=gain_in.at[slot + index],
                send_sem=gain_send.at[0],
                recv_sem=gain_recv.at[number],
                device_id=peer,
                device_id_type=pl.DeviceIdType.MESH,
            )
            copy.start()
        if number == 0:
            for head in range(heads - HELD, heads):
                send_out(head)
        wait_bytes(gain_in.at[pl.ds(slot, len(peers))], gain_recv.at[number])
        for index in range(len(peers)):
            gain = gain + gain_in[slot + index]
        slot += len(peers)
    gain_ref[...] = gain
    wait_bytes(gain_in, gain_send.at[0])
    wait_bytes(arrived.at[pl.ds(0, seq_count - 1)], in_send.at[0])
    wait_bytes(outgoing.at[0], own_out_sem.at[0])
    wait_bytes(outgoing.at[pl.ds(0, seq_count - 1)], out_send.at[0])
    wait_bytes(outgoing.at[pl.ds(0, seq_count - 1)], out_recv.at[0])


def place_kernel(seq_count, span, img, txt, land_ref, gain_ref, *refs):
    outs, sems = refs[:-1], refs[-1]
    for j in range(seq_count):
        lanes = pl.ds(j * span, span)
        for kind in range(3):
            for out, first, count in ((outs[kind], 0, img), (outs[3 + kind], img, txt)):
                pltpu.make_async_copy(
                    land_ref.at[j, kind, pl.ds(first, count)], out.at[0, :, lanes], sems.at[0]
                ).start()
    for n in range(2):
        pltpu.make_async_copy(gain_ref.at[pl.ds(n, 1)], outs[6 + n], sems.at[1]).start()
    wait_bytes(land_ref, sems.at[0])
    wait_bytes(gain_ref, sems.at[1])


def local(seq_count, iq, ik, iv, idt, tq, tk, tv, td, q_gain, k_gain):
    img, lanes = iq.shape[1], iq.shape[2]
    txt = tq.shape[1]
    rows = img + txt
    heads = lanes // HEAD_DIM // seq_count
    span = heads * HEAD_DIM
    sent = 2 * rows + 2 * img
    peers = seq_count * DP_PARTS[0] - 1 + sum(size - 1 for size in DP_PARTS[1:])
    tokens = [
        pltpu.with_memory_space_constraint(x, pltpu.HBM)
        for x in (iq, ik, iv, idt, tq, tk, tv, td, q_gain[None], k_gain[None])
    ]
    hbm = pl.BlockSpec(memory_space=pltpu.HBM)
    vmem = pl.BlockSpec(memory_space=pltpu.VMEM)
    dma = pltpu.SemaphoreType.DMA
    land, gain = pl.pallas_call(
        functools.partial(exchange_kernel, seq_count, heads, img, txt),
        out_shape=(
            pltpu.VMEM((seq_count, 3, rows, span), BF16),
            pltpu.VMEM((2, HEAD_DIM), F32),
        ),
        in_specs=[hbm] * 10,
        out_specs=(vmem, vmem),
        scratch_shapes=[
            pltpu.VMEM((seq_count, sent, span), BF16),
            pltpu.VMEM((seq_count, heads, sent, HEAD_DIM), BF16),
            pltpu.VMEM((seq_count * txt, span), BF16),
            pltpu.VMEM((seq_count * txt, span), BF16),
            pltpu.VMEM((seq_count, heads, 3, rows, HEAD_DIM), BF16),
            pltpu.VMEM((seq_count, rows, HEAD_DIM), BF16),
            pltpu.VMEM((seq_count, rows, HEAD_DIM), BF16),
            pltpu.VMEM((seq_count * rows, HEAD_DIM), F32),
            pltpu.VMEM((seq_count * rows, HEAD_DIM), F32),
            pltpu.VMEM((len(DP_PARTS), 2, HEAD_DIM), F32),
            pltpu.VMEM((peers, 2, HEAD_DIM), F32),
            dma((seq_count,)),
            dma((4 + heads,)),
            dma((1,)),
            dma((heads,)),
            dma((1,)),
            dma((1,)),
            dma((1,)),
            dma((1,)),
            dma((len(DP_PARTS),)),
            pltpu.VMEM((2, HEAD_DIM), F32),
            pltpu.SemaphoreType.REGULAR((sum(DP_PARTS[part] // 2 - 1 for part in RINGS),)),
        ],
        compiler_params=pltpu.CompilerParams(collective_id=0, has_side_effects=True, vmem_limit_bytes=40 << 20),
        name="exchange",
    )(*tokens)
    big = jax.ShapeDtypeStruct((1, img, lanes), BF16)
    small = jax.ShapeDtypeStruct((1, txt, lanes), BF16)
    row = jax.ShapeDtypeStruct((1, HEAD_DIM), F32)
    placed = pl.pallas_call(
        functools.partial(place_kernel, seq_count, span, img, txt),
        out_shape=(big,) * 3 + (small,) * 3 + (row,) * 2,
        in_specs=[vmem] * 2,
        out_specs=(hbm,) * 8,
        scratch_shapes=[dma((2,))],
        compiler_params=pltpu.CompilerParams(vmem_limit_bytes=4 << 20),
        name="place",
    )(*(pltpu.with_memory_space_constraint(x, pltpu.VMEM) for x in (land, gain)))
    return (*placed[:6], placed[6][0], placed[7][0])


def solution(mesh):
    split = P("dp", "seq", None)
    whole = P("dp", None, None)
    return jax.shard_map(
        functools.partial(local, mesh.shape["seq"]),
        mesh=mesh,
        in_specs=(split,) * 5 + (whole,) * 2 + (split, P(), P()),
        out_specs=(split,) * 6 + (P(), P()),
        check_vma=False,
    )
```

```python
import functools

import jax
import jax.numpy as jnp
from jax import lax
from jax.experimental import pallas as pl
from jax.experimental.pallas import tpu as pltpu
from jax.sharding import PartitionSpec as P

HEAD_DIM = 128
EPSILON = 1e-06
LOG2E = 1.4426950408889634
DP_PARTS = (3, 4, 8, 2)
RINGS = (1, 2)
BF16 = jnp.bfloat16
F32 = jnp.float32


def axis_peers(part):
    stride = 1
    for size in DP_PARTS[part + 1 :]:
        stride *= size
    size = DP_PARTS[part]
    index = lax.axis_index("dp")
    place = lax.rem(index // stride, size)
    base = index - place * stride
    return [{"dp": base + lax.rem(place + step, size) * stride} for step in range(1, size)]


def column_peers(seq_count):
    me = lax.axis_index("seq")
    own = [{"dp": lax.axis_index("dp")}] + axis_peers(0)
    return [
        {**lower, "seq": lax.rem(me + step, seq_count)}
        for step in range(seq_count)
        for number, lower in enumerate(own)
        if step or number
    ]


def dot_nt(a, b):
    return lax.dot_general(a, b, (((1,), (1,)), ((), ())), preferred_element_type=F32)


def dot_nn(a, b):
    return lax.dot_general(a, b, (((1,), (0,)), ((), ())), preferred_element_type=F32)


def dot_tn(a, b):
    return lax.dot_general(a, b, (((0,), (0,)), ((), ())), preferred_element_type=F32)


def inverse_rms(x):
    return lax.rsqrt(jnp.mean(x * x, axis=-1, keepdims=True) + EPSILON)


def norm_pull(x, gain, upstream):
    inverse = inverse_rms(x)
    unit = x * inverse
    scaled = upstream * gain
    along = jnp.mean(scaled * unit, axis=-1, keepdims=True)
    return inverse * (scaled - unit * along), upstream * unit


def wait_bytes(ref, sem):
    pltpu.make_async_copy(ref, ref, sem).wait()


def exchange_kernel(
    seq_count,
    heads,
    img,
    txt,
    iq_ref,
    ik_ref,
    iv_ref,
    id_ref,
    tq_ref,
    tk_ref,
    tv_ref,
    td_ref,
    qg_ref,
    kg_ref,
    land_ref,
    gain_ref,
    stage,
    arrived,
    text_k,
    text_v,
    outgoing,
    keys,
    values,
    key_acc,
    value_acc,
    gain_src,
    gain_in,
    stage_sem,
    own_sem,
    in_send,
    in_recv,
    out_send,
    out_recv,
    own_out_sem,
    gain_send,
    gain_recv,
    gains,
    hello,
):
    me = lax.axis_index("seq")
    rows = img + txt
    span = heads * HEAD_DIM
    scale = HEAD_DIM ** (-0.5)
    offsets = range(1, seq_count)
    seq_peers = [lax.rem(me + step, seq_count) for step in offsets]
    stages = [column_peers(seq_count), axis_peers(3), axis_peers(1), axis_peers(2)]
    near = [(axis_peers(part)[0], axis_peers(part)[-1]) for part in RINGS]
    greeted = column_peers(seq_count) + axis_peers(3) + [peer for pair in near for peer in pair]
    barrier = pltpu.get_barrier_semaphore()
    def fetch(owner, target, sem):
        lanes = pl.ds(pl.multiple_of(owner * span, HEAD_DIM), span)
        row = 0
        for source, count in (
            (iq_ref, img),
            (tq_ref, txt),
            (id_ref, img),
            (td_ref, txt),
            (ik_ref, img),
            (iv_ref, img),
        ):
            pltpu.make_async_copy(
                source.at[0, :, lanes], target.at[pl.ds(row, count), :], sem
            ).start()
            row += count

    for step in (2, 1, 3):
        fetch(seq_peers[step - 1], stage.at[step], stage_sem.at[step])
    for peer in greeted:
        pl.semaphore_signal(barrier, inc=1, device_id=peer, device_id_type=pl.DeviceIdType.MESH)
    def in_copy(head, step):
        lanes = pl.ds(pl.multiple_of(head * HEAD_DIM, HEAD_DIM), HEAD_DIM)
        return pltpu.make_async_remote_copy(
            src_ref=stage.at[step, :, lanes],
            dst_ref=arrived.at[me, head],
            send_sem=in_send.at[0],
            recv_sem=in_recv.at[head],
            device_id={"seq": lax.rem(me + step, seq_count)},
            device_id_type=pl.DeviceIdType.MESH,
        )

    def out_copy(head, step):
        lanes = pl.ds(pl.multiple_of(head * HEAD_DIM, HEAD_DIM), HEAD_DIM)
        peer = lax.rem(me + step, seq_count)
        return pltpu.make_async_remote_copy(
            src_ref=outgoing.at[peer, head],
            dst_ref=land_ref.at[me, :, :, lanes],
            send_sem=out_send.at[0],
            recv_sem=out_recv.at[0],
            device_id={"seq": peer},
            device_id_type=pl.DeviceIdType.MESH,
        )

    def own_in(head):
        lanes = pl.ds(pl.multiple_of(head * HEAD_DIM, HEAD_DIM), HEAD_DIM)
        return pltpu.make_async_copy(
            stage.at[0, :, lanes], arrived.at[me, head], own_sem.at[4 + head]
        )

    def own_out(head):
        lanes = pl.ds(pl.multiple_of(head * HEAD_DIM, HEAD_DIM), HEAD_DIM)
        return pltpu.make_async_copy(
            outgoing.at[me, head], land_ref.at[me, :, :, lanes], own_out_sem.at[0]
        )

    def send_out():
        half = seq_count // 2
        for group in (range(half), range(half, seq_count)):
            for head in range(heads):
                for peer in group:

                    @pl.when(me != peer)
                    def _(head=head, peer=peer):
                        out_copy(head, lax.rem(peer - me + seq_count, seq_count)).start()

        for head in range(heads):
            own_out(head).start()

    def send_in(head, carry):
        for step in (2, 1, 3):
            in_copy(head, step).start()
        return carry

    def staged(step):
        wait_bytes(stage.at[step], stage_sem.at[step])

    staged(2)
    pl.semaphore_wait(barrier, len(greeted))
    in_copy(0, 2).start()
    for step in (1, 3):
        staged(step)
        in_copy(0, step).start()
    lax.fori_loop(1, heads, send_in, 0)
    fetch(me, stage.at[0], stage_sem.at[0])
    my_lanes = pl.ds(pl.multiple_of(me * span, HEAD_DIM), span)
    text_copies = (
        pltpu.make_async_copy(tk_ref.at[0, :, my_lanes], text_k, own_sem.at[0]),
        pltpu.make_async_copy(tv_ref.at[0, :, my_lanes], text_v, own_sem.at[1]),
        pltpu.make_async_copy(qg_ref, gains.at[pl.ds(0, 1)], own_sem.at[2]),
        pltpu.make_async_copy(kg_ref, gains.at[pl.ds(1, 1)], own_sem.at[3]),
    )
    for copy in text_copies:
        copy.start()

    row = 0
    for pair, part in zip(near, RINGS):
        for _ in range(DP_PARTS[part] // 2 - 1):
            for peer in pair:
                pl.semaphore_signal(
                    hello.at[row], inc=1, device_id=peer, device_id_type=pl.DeviceIdType.MESH
                )
            pl.semaphore_wait(hello.at[row], len(pair))
            row += 1
    staged(0)
    for copy in text_copies:
        copy.wait()

    def move_own(head, carry):
        own_in(head).start()
        return carry

    lax.fori_loop(0, heads, move_own, 0)
    q_gain = gains[0:1]
    k_gain = gains[1:2]
    do_row, k_row, v_row = rows, 2 * rows, 2 * rows + img

    def one_head(head, carry):
        q_total, k_total = carry
        own_in(head).wait()
        wait_bytes(arrived.at[pl.ds(0, seq_count - 1), head], in_recv.at[head])
        lanes = pl.ds(pl.multiple_of(head * HEAD_DIM, HEAD_DIM), HEAD_DIM)

        def raw_keys(j):
            return jnp.concatenate(
                [
                    arrived[j, head, k_row : k_row + img, :].astype(F32),
                    text_k[j * txt : (j + 1) * txt, lanes].astype(F32),
                ],
                axis=0,
            )

        for j in range(seq_count):
            x = raw_keys(j)
            keys[j] = (x * inverse_rms(x) * k_gain).astype(BF16)
            values[j, :img] = arrived[j, head, v_row : v_row + img, :]
            values[j, img:] = text_v[j * txt : (j + 1) * txt, lanes]
        kn = keys[...].reshape(seq_count * rows, HEAD_DIM)
        vv = values[...].reshape(seq_count * rows, HEAD_DIM)
        def first_dots(j):
            xq = arrived[j, head, :rows, :].astype(F32)
            qn = (xq * inverse_rms(xq) * q_gain).astype(BF16)
            dout = arrived[j, head, do_row : do_row + rows, :]
            return qn, dot_nt(qn, kn), dot_nt(dout, vv)

        def soften(scores):
            weights = jnp.exp2((scores - jnp.max(scores, axis=-1, keepdims=True)) * (scale * LOG2E))
            prob = weights * (1.0 / jnp.sum(weights, axis=-1, keepdims=True))
            return prob, prob.astype(BF16)

        def score_gradient(j, prob, prob_b, dprob):
            dout = arrived[j, head, do_row : do_row + rows, :]
            out_b = dot_nn(prob_b, vv).astype(BF16)
            delta = jnp.sum(dout.astype(F32) * out_b.astype(F32), axis=-1, keepdims=True)
            return (prob * (dprob - delta) * scale).astype(BF16)

        def value_terms(j, prob_b):
            dout = arrived[j, head, do_row : do_row + rows, :]
            value_part = dot_tn(prob_b, dout).astype(BF16).astype(F32)
            value_acc[...] = value_part if j == 0 else value_acc[...] + value_part

        def last_dots(j, qn, dscore):
            key_part = dot_tn(dscore, qn).astype(BF16).astype(F32)
            key_acc[...] = key_part if j == 0 else key_acc[...] + key_part
            xq = arrived[j, head, :rows, :].astype(F32)
            dx, terms = norm_pull(xq, q_gain, dot_nn(dscore, kn))
            outgoing[j, head, 0] = dx.astype(BF16)
            return jnp.sum(terms, axis=0, keepdims=True)

        blocks, softs, dscores = {}, {}, {}
        for step, j in (("first", 0), ("soft", 0), ("first", 1), ("score", 0), ("value", 0), ("soft", 1), ("first", 2), ("last", 0), ("score", 1), ("value", 1), ("soft", 2), ("first", 3), ("last", 1), ("score", 2), ("value", 2), ("soft", 3), ("last", 2), ("score", 3), ("value", 3), ("last", 3)):
            if step == "first":
                blocks[j] = first_dots(j)
            elif step == "soft":
                softs[j] = soften(blocks[j][1])
            elif step == "score":
                dscores[j] = score_gradient(j, *softs[j], blocks[j][2])
            elif step == "value":
                value_terms(j, softs[j][1])
            else:
                q_total += last_dots(j, blocks[j][0], dscores[j])
        for j in range(seq_count):
            dx, terms = norm_pull(raw_keys(j), k_gain, key_acc[j * rows : (j + 1) * rows])
            outgoing[j, head, 1] = dx.astype(BF16)
            outgoing[j, head, 2] = value_acc[j * rows : (j + 1) * rows].astype(BF16)
            k_total += jnp.sum(terms, axis=0, keepdims=True)

        return q_total, k_total

    zero = jnp.zeros((1, HEAD_DIM), F32)
    q_total, k_total = lax.fori_loop(0, heads, one_head, (zero, zero))
    gain = jnp.concatenate([q_total, k_total], axis=0)
    slot = 0
    for number, peers in enumerate(stages):
        gain_src[number] = gain
        for index, peer in enumerate(peers):
            copy = pltpu.make_async_remote_copy(
                src_ref=gain_src.at[number],
                dst_ref=gain_in.at[slot + index],
                send_sem=gain_send.at[0],
                recv_sem=gain_recv.at[number],
                device_id=peer,
                device_id_type=pl.DeviceIdType.MESH,
            )
            copy.start()
        if number == 0:
            send_out()
        wait_bytes(gain_in.at[pl.ds(slot, len(peers))], gain_recv.at[number])
        for index in range(len(peers)):
            gain = gain + gain_in[slot + index]
        slot += len(peers)
    gain_ref[...] = gain
    wait_bytes(gain_in, gain_send.at[0])
    wait_bytes(arrived.at[pl.ds(0, seq_count - 1)], in_send.at[0])
    wait_bytes(outgoing.at[0], own_out_sem.at[0])
    wait_bytes(outgoing.at[pl.ds(0, seq_count - 1)], out_send.at[0])
    wait_bytes(outgoing.at[pl.ds(0, seq_count - 1)], out_recv.at[0])


def place_kernel(seq_count, span, img, txt, land_ref, gain_ref, *refs):
    outs, sems = refs[:-1], refs[-1]
    for j in range(seq_count):
        lanes = pl.ds(j * span, span)
        for kind in range(3):
            for out, first, count in ((outs[kind], 0, img), (outs[3 + kind], img, txt)):
                pltpu.make_async_copy(
                    land_ref.at[j, kind, pl.ds(first, count)], out.at[0, :, lanes], sems.at[0]
                ).start()
    for n in range(2):
        pltpu.make_async_copy(gain_ref.at[pl.ds(n, 1)], outs[6 + n], sems.at[1]).start()
    wait_bytes(land_ref, sems.at[0])
    wait_bytes(gain_ref, sems.at[1])


def local(seq_count, iq, ik, iv, idt, tq, tk, tv, td, q_gain, k_gain):
    img, lanes = iq.shape[1], iq.shape[2]
    txt = tq.shape[1]
    rows = img + txt
    heads = lanes // HEAD_DIM // seq_count
    span = heads * HEAD_DIM
    sent = 2 * rows + 2 * img
    peers = seq_count * DP_PARTS[0] - 1 + sum(size - 1 for size in DP_PARTS[1:])
    tokens = [
        pltpu.with_memory_space_constraint(x, pltpu.HBM)
        for x in (iq, ik, iv, idt, tq, tk, tv, td, q_gain[None], k_gain[None])
    ]
    hbm = pl.BlockSpec(memory_space=pltpu.HBM)
    vmem = pl.BlockSpec(memory_space=pltpu.VMEM)
    dma = pltpu.SemaphoreType.DMA
    land, gain = pl.pallas_call(
        functools.partial(exchange_kernel, seq_count, heads, img, txt),
        out_shape=(
            pltpu.VMEM((seq_count, 3, rows, span), BF16),
            pltpu.VMEM((2, HEAD_DIM), F32),
        ),
        in_specs=[hbm] * 10,
        out_specs=(vmem, vmem),
        scratch_shapes=[
            pltpu.VMEM((seq_count, sent, span), BF16),
            pltpu.VMEM((seq_count, heads, sent, HEAD_DIM), BF16),
            pltpu.VMEM((seq_count * txt, span), BF16),
            pltpu.VMEM((seq_count * txt, span), BF16),
            pltpu.VMEM((seq_count, heads, 3, rows, HEAD_DIM), BF16),
            pltpu.VMEM((seq_count, rows, HEAD_DIM), BF16),
            pltpu.VMEM((seq_count, rows, HEAD_DIM), BF16),
            pltpu.VMEM((seq_count * rows, HEAD_DIM), F32),
            pltpu.VMEM((seq_count * rows, HEAD_DIM), F32),
            pltpu.VMEM((len(DP_PARTS), 2, HEAD_DIM), F32),
            pltpu.VMEM((peers, 2, HEAD_DIM), F32),
            dma((seq_count,)),
            dma((4 + heads,)),
            dma((1,)),
            dma((heads,)),
            dma((1,)),
            dma((1,)),
            dma((1,)),
            dma((1,)),
            dma((len(DP_PARTS),)),
            pltpu.VMEM((2, HEAD_DIM), F32),
            pltpu.SemaphoreType.REGULAR((sum(DP_PARTS[part] // 2 - 1 for part in RINGS),)),
        ],
        compiler_params=pltpu.CompilerParams(collective_id=0, has_side_effects=True, vmem_limit_bytes=40 << 20),
        name="exchange",
    )(*tokens)
    big = jax.ShapeDtypeStruct((1, img, lanes), BF16)
    small = jax.ShapeDtypeStruct((1, txt, lanes), BF16)
    row = jax.ShapeDtypeStruct((1, HEAD_DIM), F32)
    placed = pl.pallas_call(
        functools.partial(place_kernel, seq_count, span, img, txt),
        out_shape=(big,) * 3 + (small,) * 3 + (row,) * 2,
        in_specs=[vmem] * 2,
        out_specs=(hbm,) * 8,
        scratch_shapes=[dma((2,))],
        compiler_params=pltpu.CompilerParams(vmem_limit_bytes=4 << 20),
        name="place",
    )(*(pltpu.with_memory_space_constraint(x, pltpu.VMEM) for x in (land, gain)))
    return (*placed[:6], placed[6][0], placed[7][0])


def solution(mesh):
    split = P("dp", "seq", None)
    whole = P("dp", None, None)
    return jax.shard_map(
        functools.partial(local, mesh.shape["seq"]),
        mesh=mesh,
        in_specs=(split,) * 5 + (whole,) * 2 + (split, P(), P()),
        out_specs=(split,) * 6 + (P(), P()),
        check_vma=False,
    )
```
